32 devices in a mesh: dp: 4 (over z), stage: 2 (over y), tp: 4 (over x, core).
Axes of the slice: x: 2, y: 2, z: 4, core: 2. Of those that a mesh axis runs over, the one named last changes fastest.
Arguments:
- act_in: bfloat16 [2, 16, 28, 28, 512], P('stage', ('dp', 'tp'))
- w_conv: bfloat16 [2, 3, 3, 512, 512], P('stage', None, None, 'tp')
- w_short: bfloat16 [2, 512, 512], P('stage', 'tp')
- gamma: float32 [2, 512], P('stage', 'tp')
- beta: float32 [2, 512], P('stage', 'tp')
- gamma_s: float32 [2, 512], P('stage', 'tp')
- grad_z: bfloat16 [2, 16, 28, 28, 512], P('stage', 'dp', None, None, 'tp')
Outputs:
- output 1: bfloat16 [2, 16, 28, 28, 512], P('stage', 'dp', None, None, 'tp')
- output 2: bfloat16 [2, 16, 28, 28, 512], P('stage', ('dp', 'tp'))
- output 3: float32 [2, 3, 3, 512, 512], P('stage', None, None, 'tp')
- output 4: float32 [2, 512, 512], P('stage', 'tp')
All inputs are finite; a program needn't handle non-finite values.
Results may differ from the reference program's by a relative error of at most 0.00599.
Values are sent between devices in bfloat16 or wider.
A program may use at most 1 GiB of HBM per device.

```python
import jax
import jax.numpy as jnp
from jax import lax

NUM_STAGES = 2
BATCH_ALL = 16
BLOCK_IMGS = 1
IMG_HEIGHT = 28
IMG_WIDTH = 28
CH_IN = 512
CH_OUT = 512


def place_slot(array_in, slot_index):
    pad_before = jnp.zeros((slot_index,) + array_in.shape, array_in.dtype)
    pad_after = jnp.zeros((NUM_STAGES - slot_index - 1,) + array_in.shape, array_in.dtype)
    return jnp.concatenate([pad_before, array_in[None], pad_after], axis=0)


def setup_inputs(seed: int = 0) -> dict:
    key_list = jax.random.split(jax.random.key(seed), 7)
    act_draw = jax.random.normal(key_list[0], (BATCH_ALL, IMG_HEIGHT, IMG_WIDTH, CH_IN), jnp.float32)
    conv_draw = jax.random.normal(key_list[1], (3, 3, CH_IN, CH_OUT), jnp.float32) * (9 * CH_IN) ** -0.5
    short_draw = jax.random.normal(key_list[2], (CH_IN, CH_OUT), jnp.float32) * CH_IN ** -0.5
    gamma_draw = jax.random.uniform(key_list[3], (CH_OUT,), jnp.float32, 0.5, 1.5)
    beta_draw = 0.5 * jax.random.normal(key_list[4], (CH_OUT,), jnp.float32)
    gamma_s_draw = jax.random.uniform(key_list[5], (CH_OUT,), jnp.float32, 0.5, 1.5)
    grad_draw = jax.random.normal(key_list[6], (BATCH_ALL, IMG_HEIGHT, IMG_WIDTH, CH_OUT), jnp.float32)
    return {
        "act_in": place_slot(act_draw.astype(jnp.bfloat16), 0),
        "w_conv": place_slot(conv_draw.astype(jnp.bfloat16), 1),
        "w_short": place_slot(short_draw.astype(jnp.bfloat16), 1),
        "gamma": place_slot(gamma_draw, 1),
        "beta": place_slot(beta_draw, 1),
        "gamma_s": place_slot(gamma_s_draw, 1),
        "grad_z": place_slot(grad_draw.astype(jnp.bfloat16), 1),
    }


def reference(act_in, w_conv, w_short, gamma, beta, gamma_s, grad_z):
    kernel = w_conv[1].astype(jnp.float32)
    short_w = w_short[1].astype(jnp.float32)
    scale_main = gamma[1]
    shift_main = beta[1]
    scale_short = gamma_s[1]
    num_blocks = BATCH_ALL // BLOCK_IMGS
    act_blocks = act_in[0].reshape(num_blocks, BLOCK_IMGS, IMG_HEIGHT, IMG_WIDTH, CH_IN)
    grad_blocks = grad_z[1].reshape(num_blocks, BLOCK_IMGS, IMG_HEIGHT, IMG_WIDTH, CH_OUT)

    def linear_part(images, conv_w, proj_w):
        pre_act = lax.conv_general_dilated(images, conv_w, (1, 1), "SAME", dimension_numbers=("NHWC", "HWIO", "NHWC"))
        short_out = jnp.einsum("nhwc,co->nhwo", images, proj_w)
        return pre_act, short_out

    def block_step(acc_pair, block_in):
        act_blk, grad_blk = block_in
        (pre_act, short_out), pull_back = jax.vjp(linear_part, act_blk.astype(jnp.float32), kernel, short_w)
        mixed_sum = pre_act * scale_main + shift_main + short_out * scale_short
        z_blk = jnp.maximum(mixed_sum, 0.0).astype(jnp.bfloat16)
        mask_pos = mixed_sum > 0.0
        grad_wide = grad_blk.astype(jnp.float32)
        g_main = jnp.where(mask_pos, grad_wide * scale_main, 0.0).astype(jnp.bfloat16)
        g_short = jnp.where(mask_pos, grad_wide * scale_short, 0.0).astype(jnp.bfloat16)
        grad_images, grad_conv, grad_proj = pull_back((g_main.astype(jnp.float32), g_short.astype(jnp.float32)))
        new_acc = (acc_pair[0] + grad_conv, acc_pair[1] + grad_proj)
        return new_acc, (z_blk, grad_images.astype(jnp.bfloat16))

    acc_init = (jnp.zeros((3, 3, CH_IN, CH_OUT), jnp.float32), jnp.zeros((CH_IN, CH_OUT), jnp.float32))
    (dw_sum, dws_sum), (z_blocks, dx_blocks) = lax.scan(block_step, acc_init, (act_blocks, grad_blocks))
    z_all = z_blocks.reshape(BATCH_ALL, IMG_HEIGHT, IMG_WIDTH, CH_OUT)
    dx_all = dx_blocks.reshape(BATCH_ALL, IMG_HEIGHT, IMG_WIDTH, CH_IN)
    return (place_slot(z_all, 1), place_slot(dx_all, 0), place_slot(dw_sum, 1), place_slot(dws_sum, 1))
```

```python
import jax
import jax.numpy as jnp
from jax import lax
from jax.experimental import pallas as pl
from jax.experimental.pallas import tpu as pltpu
from jax.sharding import PartitionSpec as P

BF = jnp.bfloat16
F32 = jnp.float32
MESH = pl.DeviceIdType.MESH
B = 128
C = 4 * B
W3 = 3 * B
IMGS = 4
HW = 28
WP = 32
HT = 7
NT = 4
M = HT * WP
NCROSS = 1
R = B // 2
NEAR = (0, 2)
MAIN = 1


def lanes(k):
    return pl.ds(pl.multiple_of(k * B, B), B)


def block_kernel(act, wc, ws, gam, bet, gams, gz, z_out, dx_out, dw_out, ds_out,
                 xl, x4, xt, w4, s4, wf, dzl, wide, d4, dzm, zf, zb, g4, part, pa, re, rm, tt, ff, fo, ob, obs,
                 w0, s0, ga, gsa, g0, gp, gsp, dxb, sem):
    dp = lax.axis_index("dp")
    st = lax.axis_index("stage")
    tp = lax.axis_index("tp")
    par = lax.rem(tp, 2)
    half = tp // 2
    sib = tp + 1 - 2 * par
    nbx = lax.rem(tp + 2, IMGS)
    dia = lax.rem(sib + 2, IMGS)

    def rc(src, dst, name, *k, land=None, **dev):
        ssem, rsem = sem["s" + name], sem["r" + name]
        return pltpu.make_async_remote_copy(src_ref=src, dst_ref=dst, send_sem=ssem.at[k], recv_sem=rsem.at[land or k], device_id=dev, device_id_type=MESH)

    def local(src, dst, k):
        return pltpu.make_async_copy(src, dst, sem["l"].at[k])

    def owner(o):
        return jnp.where(o == 0, tp, jnp.where(o == 1, sib, jnp.where(o == 2, nbx, dia)))

    is_end = jnp.logical_or(dp == 0, dp == 3)
    inner = jnp.where(dp == 0, 1, 2)

    def up(k, n):
        return rc(pa.at[k, :, pl.ds(0, n)], re.at[k, :, pl.ds(0, n)], "e", k, dp=inner)

    def send_up(ks, n, p_wait):
        @pl.when(is_end)
        def _():
            for k in ks:
                p_wait(k)
                up(k, n).start()

    def all_reduce(pairs, n, p_wait, emit):
        def cols(ref, k):
            return ref.at[k, :, pl.ds(0, n)]

        @pl.when(is_end)
        def _():
            for k in range(2 * pairs):
                rc(cols(ff, k), cols(ff, k), "h", k, dp=inner).wait_recv()
                emit(k)
            for k in range(2 * pairs):
                up(k, n).wait_send()

        @pl.when(jnp.logical_not(is_end))
        def _():
            endn = jnp.where(dp == 1, 0, 3)
            midn = 3 - dp

            def mine(m):
                return 2 * m + dp - 1

            def other(m):
                return 2 * m + 2 - dp

            def e_wait(k):
                rc(cols(pa, k), cols(re, k), "e", k, dp=endn).wait_recv()

            def to_root(m):
                return rc(cols(tt, m), cols(rm, m), "m", m, dp=midn)

            def to_mid(k):
                return rc(cols(ff, k), cols(ff, k), "f", k, dp=midn)

            def to_end(k):
                return rc(cols(ff, k), cols(ff, k), "h", k, dp=endn)

            def forward_result(m):
                k = other(m)
                rc(cols(ff, k), cols(ff, k), "f", k, dp=midn).wait_recv()
                to_end(k).start()
                emit(k)

            for m in range(pairs):
                k = other(m)
                p_wait(k)
                e_wait(k)
                tt[m, :, :n] = pa[k, :, :n] + re[k, :, :n]
                to_root(m).start()
                k = mine(m)
                p_wait(k)
                e_wait(k)
                to_root(m).wait_recv()
                ff[k, :, :n] = pa[k, :, :n] + re[k, :, :n] + rm[m, :, :n]
                to_end(k).start()
                to_mid(k).start()
                emit(k)
                if m > 0:
                    forward_result(m - 1)
            forward_result(pairs - 1)
            for m in range(pairs):
                to_root(m).wait_send()
                to_mid(mine(m)).wait_send()
                to_end(mine(m)).wait_send()
                to_end(other(m)).wait_send()

    @pl.when(st == 1)
    def _():
        def own_w(k, dst_k):
            return wc.at[:, :, :, lanes(k)], w4.at[:, :, lanes(dst_k)]

        def own_s(k, dst_k):
            return ws.at[:, lanes(k)], s4.at[lanes(dst_k)]

        loads = [local(gz, dzl, 0), local(*own_w(tp, tp), 1), local(*own_s(tp, tp), 2)]
        for c in loads:
            c.start()

        def w_copy(o):
            return rc(*own_w(owner(o), tp), "w", o, tp=owner(o))

        def s_copy(o):
            return rc(*own_s(owner(o), tp), "v", o, tp=owner(o))

        odd = lax.rem(dp, 2)
        peer = dp + 1 - 2 * odd

        def w_half(o, k, h):
            rows = pl.ds(k * B + h * R, R)
            return w4.at[:, :, rows], s4.at[rows]

        def far_copies(o):
            k = owner(o)
            mine = pl.ds(odd * R, R)
            dst_w, dst_s = w_half(o, tp, odd)
            return rc(wc.at[:, :, mine, lanes(k)], dst_w, "w", o, tp=k), rc(ws.at[mine, lanes(k)], dst_s, "v", o, tp=k)

        def far_recv(o):
            dst_w, dst_s = w_half(o, owner(o), odd)
            return rc(dst_w, dst_w, "w", o, tp=owner(o)), rc(dst_s, dst_s, "v", o, tp=owner(o))

        def peer_copies(o, h):
            dst_w, dst_s = w_half(o, owner(o), h)
            return rc(dst_w, dst_w, "i", o, dp=peer), rc(dst_s, dst_s, "j", o, dp=peer)

        far = (2, 3)
        w_sends = [*far_copies(2), *far_copies(3), w_copy(1), s_copy(1)]
        for c in w_sends:
            c.start()

        quarters = [rc(wc.at[i], w0.at[i, :, tp], "a", i, stage=0) for i in range(3)]
        quarters.append(rc(ws, s0.at[tp], "a", 3, stage=0))
        for o in range(IMGS):
            quarters.append(rc(gam, ga.at[tp], "y", o, stage=0, tp=owner(o)))
            quarters.append(rc(gams, gsa.at[tp], "u", o, stage=0, tp=owner(o)))
        for c in quarters:
            c.start()

        edge = jnp.zeros((WP, C), BF)
        for o in range(IMGS):
            for r in (0, HW + 1):
                x4[o, r] = edge
                g4[o, r] = edge
        x4[:, :, 24:, :] = jnp.zeros((IMGS, HW + 2, 8, C), BF)
        d4[:, :, 24:, :] = jnp.zeros((IMGS, HW, 8, B), BF)
        for i in NEAR:
            wf[i, :, W3:] = jnp.zeros((C, B), BF)

        loads[0].wait()
        wide[...] = dzl[...].astype(F32)

        def split_rows(h, c):
            for o in range(IMGS):
                d4[o, h, :HW, :] = wide[pl.ds(h * HW * IMGS + o, HW, stride=IMGS), :].astype(BF)
            return c

        lax.fori_loop(0, HW, split_rows, 0)

        scale_main = gam[...]
        shift_main = bet[...]
        scale_short = gams[...]

        def rows(img, k):
            return xl.at[img, pl.ds(k * HT, HT)]

        def land(o, k):
            img = owner(o)
            ref = rows(img, k)
            if o == 0:
                rc(ref, ref, "a", k, stage=0).wait_recv()
                rc(ref, ref, "b", k, tp=sib).start()

                @pl.when(k >= NCROSS)
                def _():
                    rc(ref, ref, "c", k, tp=nbx).start()
            elif o == 1:
                rc(ref, ref, "b", k, tp=sib).wait_recv()
            elif o == 2:
                rc(ref, ref, "c", k, tp=nbx).wait_recv()
                rc(ref, ref, "d", k, tp=sib).start()
            else:
                rc(ref, ref, "d", k, tp=sib).wait_recv()
            for r in range(HT):
                h = k * HT + r
                x4[img, 1 + h, :HW, :] = xl[img, h]

        def weights():
            for c in loads[1:]:
                c.wait()
            rc(*own_w(sib, sib), "w", 1, tp=sib).wait_recv()
            rc(*own_s(sib, sib), "v", 1, tp=sib).wait_recv()
            for o in far:
                for c in peer_copies(o, 1 - odd):
                    c.wait_recv()
            for i in range(3):
                for j in range(3):
                    wf[i, :, j * B:(j + 1) * B] = w4[i, j]
            wf[MAIN, :, W3:] = s4[...]

        def g_copy(o):
            k = owner(o)
            return rc(dzm.at[k], g0.at[tp], "g", o, stage=0, tp=k)

        def tile(img, t):
            h0 = t * HT
            acc = None
            for i in range(3):
                d = jnp.dot(x4[img, pl.ds(h0 + i, HT)].reshape(M, C), wf[i], preferred_element_type=F32)
                acc = d if acc is None else acc + d
            pre = pltpu.roll(acc[:, :B], 1, 0) + acc[:, B:2 * B] + pltpu.roll(acc[:, 2 * B:W3], M - 1, 0)
            mixed = pre * scale_main + shift_main + acc[:, W3:] * scale_short
            z = jnp.maximum(mixed, 0.0)
            for r in range(HT):
                zf[pl.ds((h0 + r) * HW * IMGS + img, HW, stride=IMGS), :] = z[r * WP:r * WP + HW]
            dz = d4[img, pl.ds(h0, HT)].reshape(M, B).astype(F32)
            dz = jnp.where(mixed > 0.0, dz, 0.0)
            dzm[img, pl.ds(h0, HT)] = dz.astype(BF).reshape(HT, WP, B)[:, :HW, :]
            g = dz * scale_main
            for j, val in enumerate((pltpu.roll(g, M - 1, 0), g, pltpu.roll(g, 1, 0), dz * scale_short)):
                g4[img, pl.ds(1 + h0, HT), :, j * B:(j + 1) * B] = val.astype(BF).reshape(HT, WP, B)

        def step(t, c):
            @pl.when(t == 0)
            def _():
                for o in far:
                    for c in far_recv(o):
                        c.wait_recv()
                    for c in peer_copies(o, odd):
                        c.start()

            for o in range(IMGS):
                k = t - o

                @pl.when(jnp.logical_and(k >= 0, k < NT))
                def _():
                    land(o, k)

            @pl.when(t == 1)
            def _():
                weights()

            def per_image(o, c2):
                img = owner(o)
                k = t - o - 1

                @pl.when(jnp.logical_and(k >= 0, k < NT))
                def _():
                    tile(img, k)

                @pl.when(k == NT - 1)
                def _():
                    @pl.when(o < 2)
                    def _():
                        g_copy(o).start()

                    xt[img] = x4[img, 1:HW + 1].reshape(HW * WP, C).T

                return c2

            return lax.fori_loop(0, IMGS, per_image, c)

        with jax.named_scope("s1_fwd"):
            lax.fori_loop(0, 2 * NT, step, 0)

        def part_near(k, q):
            return rc(part.at[k, :, pl.ds(0, W3)], pa.at[k, :, pl.ds(0, W3)], "p", k, tp=q)

        def part_main(k):
            return rc(part.at[4 * IMGS + k], pa.at[k], "q", k, stage=0)

        def weight_grad(i, n, done):
            def half_step(e, c):
                hx = jnp.where(e == 0, 1 - half, half)
                c0 = pl.multiple_of(hx * 2 * B, 2 * B)
                acc = None
                for img in range(IMGS):
                    rhs = g4[img, 2 - i:2 - i + HW, :, :n].reshape(HW * WP, n)
                    d = jnp.dot(xt[img, pl.ds(c0, 2 * B), :], rhs, preferred_element_type=F32)
                    acc = d if acc is None else acc + d
                for p in range(2):
                    for h in range(2):
                        r = p * B + h * R
                        done(e, p, h, 2 * hx + p, acc[r:r + R])
                return c

            lax.fori_loop(0, 2, half_step, 0)

        def near_chunk(e, p, h, idx):
            return 4 * idx + 4 * len(NEAR) * (1 - e) + 2 * h + lax.rem(p + par, 2)

        def near_done(idx):
            def done(e, p, h, q, val):
                k = near_chunk(e, p, h, idx)

                @pl.when(q == tp)
                def _():
                    pa[k, :, :W3] = val

                @pl.when(q != tp)
                def _():
                    part[k, :, :W3] = val
                    part_near(k, q).start()

            return done

        def main_done(e, p, h, q, val):
            k = 4 * e + 2 * h + p
            part[4 * IMGS + k] = val
            part_main(k).start()

        def p_wait(k):
            @pl.when(jnp.logical_or(k >= 4 * len(NEAR), lax.rem(k, 2) == 1))
            def _():
                part_near(k, sib).wait_recv()

        with jax.named_scope("s1_dw"):
            weight_grad(NEAR[0], W3, near_done(0))
            send_up((0, 2), W3, p_wait)
            weight_grad(MAIN, C, main_done)
            send_up((1, 3), W3, p_wait)
            weight_grad(NEAR[1], W3, near_done(1))
            send_up(range(4, 8), W3, p_wait)
            for o in far:
                g_copy(o).start()
            zb[...] = zf[...].astype(BF)
            z_copy = local(zb, z_out, 4)
            z_copy.start()

        def place(i, src, ref, k, h):
            for j in range(3):
                ob[i, j, h * R:(h + 1) * R, lanes(src)] = ref[k, :, j * B:(j + 1) * B]

        with jax.named_scope("s1_ar"):
            send_up(range(8, 16), W3, p_wait)
            all_reduce(4 * len(NEAR), W3, p_wait, lambda k: None)
        outs = [local(ob.at[i], dw_out.at[i], 5 + i) for i in range(3)]
        with jax.named_scope("s1_out"):
            for idx, i in enumerate(NEAR):
                for o in range(IMGS):
                    for h in range(2):
                        place(i, owner(o), ff, 4 * idx + 4 * len(NEAR) * (o // 2) + 2 * h + o % 2, h)
                outs[i].start()
            for h in range(2):
                for o in range(IMGS):
                    src = owner(o)
                    rc(ff.at[o], fo.at[h, src], "o", o, land=(2 * src + h,), stage=0).wait_recv()
                    place(MAIN, src, fo.at[h], src, h)
                    obs[h * R:(h + 1) * R, lanes(src)] = fo[h, src, :, W3:]
            outs[MAIN].start()
            outs.append(local(obs, ds_out, 8))
            outs[-1].start()

        for o in far:
            w_sends.extend(peer_copies(o, odd))
        for c in w_sends:
            c.wait_send()
        for c in quarters:
            c.wait_send()

        def drain(k, c):
            g_copy(k).wait_send()
            rc(rows(tp, k), rows(tp, k), "b", k, tp=sib).wait_send()
            rc(rows(nbx, k), rows(nbx, k), "d", k, tp=sib).wait_send()
            part_main(k).wait_send()
            part_main(IMGS + k).wait_send()

            @pl.when(k >= NCROSS)
            def _():
                rc(rows(tp, k), rows(tp, k), "c", k, tp=nbx).wait_send()

            return c

        lax.fori_loop(0, NT, drain, 0)
        for idx in range(len(NEAR)):
            for e in range(2):
                for p in range(2):
                    q = 2 * jnp.where(e == 0, 1 - half, half) + p

                    @pl.when(q != tp)
                    def _():
                        for h in range(2):
                            part_near(near_chunk(e, p, h, idx), q).wait_send()
        for c in (z_copy, *outs):
            c.wait()

    @pl.when(st == 0)
    def _():
        def rows(k):
            return act.at[pl.ds(k * HT, HT)], xl.at[tp, pl.ds(k * HT, HT)]

        sends = [rc(*rows(k), "a", k, stage=1) for k in range(NT)]
        sends += [rc(*rows(k), "c", k, stage=1, tp=nbx) for k in range(NCROSS)]
        for c in sends:
            c.start()

        def wref(q, k):
            return w0.at[k, :, q] if k < 3 else s0.at[q]

        def hop(name, q, k, dst):
            return rc(wref(q, k), wref(q, k), name, k, tp=dst)

        with jax.named_scope("s0_relay"):
            for k in range(NT + 1):
                if k < NT:
                    rc(wref(tp, k), wref(tp, k), "a", k, stage=1).wait_recv()
                    hop("c", tp, k, nbx).start()
                    hop("b", tp, k, sib).start()
                if k > 0:
                    hop("c", nbx, k - 1, nbx).wait_recv()
                    hop("d", nbx, k - 1, sib).start()
        edge = jnp.zeros((WP, C), BF)
        gp[0] = edge
        gp[HW + 1] = edge
        gp[:, 24:, :] = jnp.zeros((HW + 2, 8, C), BF)
        gsp[:, 24:, :] = jnp.zeros((HW, 8, C), BF)

        def p_wait(k):
            rc(pa.at[k], pa.at[k], "q", k, stage=1).wait_recv()

        def result(k):
            q = 2 * jnp.where(k < IMGS, 1 - half, half) + lax.rem(k, 2)
            h = lax.rem(k, IMGS) // 2
            return rc(ff.at[k], fo.at[h, tp], "o", k, land=(2 * tp + h,), stage=1, tp=q)

        with jax.named_scope("s0_ar"):
            send_up(range(2 * IMGS), C, p_wait)
            all_reduce(IMGS, C, p_wait, lambda k: result(k).start())

        with jax.named_scope("s0_wait"):
            for k in range(NT):
                hop("b", sib, k, sib).wait_recv()
                hop("d", dia, k, sib).wait_recv()
            for o in range(IMGS):
                q = owner(o)
                rc(gam, ga.at[q], "y", o, stage=1, tp=q).wait_recv()
                rc(gams, gsa.at[q], "u", o, stage=1, tp=q).wait_recv()
                rc(dzm.at[tp], g0.at[q], "g", o, stage=1, tp=q).wait_recv()

        def build(h, c):
            for q in range(IMGS):
                dz = g0[q, h].astype(F32)
                gp[1 + h, :HW, q * B:(q + 1) * B] = (dz * ga[q]).astype(BF)
                gsp[h, :HW, q * B:(q + 1) * B] = (dz * gsa[q]).astype(BF)
            return c

        contract = (((1,), (1,)), ((), ()))

        def dx_tile(t, c):
            h0 = t * HT
            total = None
            for j in (1, 0, 2):
                d = None
                for i in range(3):
                    lhs = gp[pl.ds(h0 + 2 - i, HT)].reshape(M, C)
                    p = lax.dot_general(lhs, w0[i, j].reshape(C, C), contract, preferred_element_type=F32)
                    d = p if d is None else d + p
                if j == 1:
                    d += lax.dot_general(gsp[pl.ds(h0, HT)].reshape(M, C), s0[...].reshape(C, C), contract, preferred_element_type=F32)
                else:
                    d = pltpu.roll(d, M - 1 if j == 0 else 1, 0)
                total = d if total is None else total + d
            dxb[pl.ds(h0, HT)] = total.astype(BF).reshape(HT, WP, C)[:, :HW, :]
            return c

        with jax.named_scope("s0_dx"):
            lax.fori_loop(0, HW, build, 0)
            lax.fori_loop(0, NT, dx_tile, 0)
        dx_copy = local(dxb, dx_out, 5)
        dx_copy.start()

        for c in sends:
            c.wait_send()
        for k in range(NT):
            hop("c", tp, k, nbx).wait_send()
            hop("b", tp, k, sib).wait_send()
            hop("d", nbx, k, sib).wait_send()
        for k in range(2 * IMGS):
            result(k).wait_send()
        dx_copy.wait()


def scratch_shapes():
    def v(*shape, dtype=BF):
        return pltpu.VMEM(shape, dtype)

    def f(*shape):
        return pltpu.VMEM(shape, F32)

    n = HW * HW * IMGS
    buffers = [
        v(IMGS, HW, HW, C),
        v(IMGS, HW + 2, WP, C),
        v(IMGS, C, HW * WP),
        v(3, 3, C, B),
        v(C, B),
        v(3, C, C),
        v(n, B),
        f(n, B),
        v(IMGS, HW, WP, B),
        v(IMGS, HW, HW, B),
        f(n, B),
        v(n, B),
        v(IMGS, HW + 2, WP, C),
        f(6 * IMGS, R, C),
        f(4 * IMGS, R, C),
        f(4 * IMGS, R, C),
        f(2 * IMGS, R, C),
        f(2 * IMGS, R, C),
        f(4 * IMGS, R, C),
        f(2, IMGS, R, C),
        f(3, 3, B, C),
        f(B, C),
        v(3, 3, IMGS, B, C),
        v(IMGS, B, C),
        f(IMGS, 1, B),
        f(IMGS, 1, B),
        v(IMGS, HW, HW, B),
        v(HW + 2, WP, C),
        v(HW, WP, C),
        v(HW, HW, C),
    ]
    sems = {}
    for names, n in (("abcdwvyugij", IMGS), ("moq", 2 * IMGS), ("efhp", 4 * IMGS)):
        for name in names:
            sems["s" + name] = n
            sems["r" + name] = n
    sems["l"] = 9
    return [*buffers, {k: pltpu.SemaphoreType.DMA((n,)) for k, n in sems.items()}]


def place_kernel(z, dx, dw, ds, z_out, dx_out, dw_out, ds_out, zb, dxb, dwb, dsb, sem_in, sem_out):
    st = lax.axis_index("stage")
    zs = (z, zb, z_out)
    xs = (dx, dxb, dx_out)
    ws = (dw, dwb, dw_out)
    ss = (ds, dsb, ds_out)

    def move(moved, zeroed):
        copies = [(pltpu.make_async_copy(a, b, sem_in.at[k]), pltpu.make_async_copy(b, c, sem_out.at[k])) for k, (a, b, c) in enumerate(moved)]
        for load, _ in copies:
            load.start()
        fills = [pltpu.make_async_copy(b, c, sem_out.at[len(moved) + k]) for k, (_, b, c) in enumerate(zeroed)]
        for (_, b, _), c in zip(zeroed, fills):
            b[...] = jnp.zeros_like(b)
            c.start()
        for load, store in copies:
            load.wait()
            store.start()
        for _, store in copies:
            store.wait()
        for c in fills:
            c.wait()

    @pl.when(st == 1)
    def _():
        move([zs, ss, ws], [xs])

    @pl.when(st == 0)
    def _():
        move([xs], [zs, ss, ws])


def solution(mesh):
    act_spec = P("stage", ("dp", "tp"), None, None, None)
    kernel_spec = P("stage", None, None, "tp", None)
    short_spec = P("stage", "tp", None)
    vec_spec = P("stage", "tp")
    grad_spec = P("stage", "dp", None, None, "tp")
    any_ = pl.BlockSpec(memory_space=pl.ANY)
    vm = pl.BlockSpec(memory_space=pltpu.VMEM)

    def device_step(act_in, w_conv, w_short, gamma, beta, gamma_s, grad_z):
        by_pixel = (0, 2, 3, 1, 4)
        grads = jnp.transpose(grad_z, by_pixel).reshape(-1, B)
        call = pl.pallas_call(
            block_kernel,
            out_shape=(
                jax.ShapeDtypeStruct(grads.shape, BF),
                jax.ShapeDtypeStruct(act_in.shape[2:], BF),
                jax.ShapeDtypeStruct(w_conv.shape[1:], F32),
                jax.ShapeDtypeStruct(w_short.shape[1:], F32),
            ),
            in_specs=[any_, any_, any_, vm, vm, vm, any_],
            out_specs=(any_, any_, any_, any_),
            scratch_shapes=scratch_shapes(),
            compiler_params=pltpu.CompilerParams(vmem_limit_bytes=64000000, has_side_effects=True),
        )
        found = call(act_in[0, 0], w_conv[0], w_short[0], gamma, beta, gamma_s, grads)
        z, dx, dw, ds = pl.pallas_call(
            place_kernel,
            out_shape=tuple(jax.ShapeDtypeStruct(a.shape, a.dtype) for a in found),
            in_specs=[any_] * 4,
            out_specs=(any_,) * 4,
            scratch_shapes=[*(pltpu.VMEM(a.shape, a.dtype) for a in found), pltpu.SemaphoreType.DMA((4,)), pltpu.SemaphoreType.DMA((4,))],
            compiler_params=pltpu.CompilerParams(vmem_limit_bytes=64000000),
        )(*found)
        z = jnp.transpose(z.reshape(1, HW, HW, IMGS, B), (0, 3, 1, 2, 4))
        return z, dx[None, None], dw[None], ds[None]

    return jax.shard_map(device_step, mesh=mesh, in_specs=(act_spec, kernel_spec, short_spec, vec_spec, vec_spec, vec_spec, grad_spec), out_specs=(grad_spec, act_spec, kernel_spec, short_spec), check_vma=False)
```

```python
import jax
import jax.numpy as jnp
from jax import lax
from jax.experimental import pallas as pl
from jax.experimental.pallas import tpu as pltpu
from jax.sharding import PartitionSpec as P

BF = jnp.bfloat16
F32 = jnp.float32
MESH = pl.DeviceIdType.MESH
B = 128
C = 4 * B
W3 = 3 * B
IMGS = 4
HW = 28
WP = 32
HT = 7
NT = 4
M = HT * WP
LAG = 8
LATE = 7
R = 32
NR = B // R
W_ROWS = 10 * B // 2
HB = B // 2
CROSS = 4
NEAR = (0, 2)
NEARS = 4 * NR * len(NEAR)
MAIN = 1


def lanes(k):
    return pl.ds(pl.multiple_of(k * B, B), B)


def block_kernel(act, wc, ws, gam, bet, gams, gz, z_out, dx_out, dw_out, ds_out,
                 xl, x4, xt, w4, s4, wf, dzl, wide, d4, dzm, zf, zb, g4, part, pa, re, rm, tt, ff, fo, ob, obs,
                 w0, s0, ga, gsa, g0, gp, gsp, dxb, sem):
    dp = lax.axis_index("dp")
    st = lax.axis_index("stage")
    tp = lax.axis_index("tp")
    par = lax.rem(tp, 2)
    half = tp // 2
    sib = tp + 1 - 2 * par
    nbx = lax.rem(tp + 2, IMGS)
    dia = lax.rem(sib + 2, IMGS)
    odd = lax.rem(dp, 2)
    peer = dp + 1 - 2 * odd

    barrier = pltpu.get_barrier_semaphore()

    def greet(**dev):
        pl.semaphore_signal(barrier, inc=1, device_id=dev, device_id_type=MESH)

    for mate in (sib, nbx, dia):
        greet(tp=mate)
        greet(stage=1 - st, tp=mate)
    greet(stage=1 - st)
    is_end = jnp.logical_or(dp == 0, dp == 3)
    inner = jnp.where(dp == 0, 1, 2)
    endn = jnp.where(dp == 1, 0, 3)
    midn = 3 - dp
    mates = 7

    @pl.when(is_end)
    def _():
        greet(dp=inner)
        pl.semaphore_wait(barrier, mates + 1)

    @pl.when(jnp.logical_not(is_end))
    def _():
        greet(dp=endn)
        greet(dp=midn)
        pl.semaphore_wait(barrier, mates + 2)

    def rc(src, dst, name, *k, land=None, **dev):
        ssem, rsem = sem["s" + name], sem["r" + name.replace("h", "e")]
        return pltpu.make_async_remote_copy(src_ref=src, dst_ref=dst, send_sem=ssem.at[0], recv_sem=rsem.at[land or k], device_id=dev, device_id_type=MESH)

    def sent(name, ref):
        pltpu.make_async_remote_copy(src_ref=ref, dst_ref=ref, send_sem=sem["s" + name].at[0], recv_sem=sem["re"].at[0], device_id={"tp": sib}, device_id_type=MESH).wait_send()

    def local(src, dst, k):
        return pltpu.make_async_copy(src, dst, sem["l"].at[k])

    def owner(o):
        return jnp.where(o == 0, tp, jnp.where(o == 1, sib, jnp.where(o == 2, nbx, dia)))

    def up(k, n):
        return rc(pa.at[k, :, pl.ds(0, n)], re.at[k, :, pl.ds(0, n)], "e", k, dp=inner)

    def arrive(k, n, emit):
        ref = ff.at[k, :, pl.ds(0, n)]
        rc(ref, ref, "h", k, dp=inner).wait_recv()
        emit(k)

    def send_up(ks, n, p_wait, lag=None, emit=None):
        @pl.when(is_end)
        def _():
            for k in ks:
                p_wait(k)
                up(k, n).start()
                if lag is not None and k >= lag:
                    arrive(k - lag, n, emit)

    def e_wait(k, n):
        rc(pa.at[k, :, pl.ds(0, n)], re.at[k, :, pl.ds(0, n)], "e", k, dp=endn).wait_recv()

    def to_root(m, n):
        return rc(tt.at[m, :, pl.ds(0, n)], rm.at[m, :, pl.ds(0, n)], "m", m, dp=midn)

    def pass_on(m, n, p_wait):
        k = 2 * m + 2 - dp
        p_wait(k)
        e_wait(k, n)
        tt[m, :, :n] = pa[k, :, :n] + re[k, :, :n]
        to_root(m, n).start()

    def all_reduce(pairs, n, p_wait, emit, outer_work=None, inner_work=None, first=0, ahead=1):
        def cols(ref, k):
            return ref.at[k, :, pl.ds(0, n)]

        @pl.when(is_end)
        def _():
            for k in range(first, 2 * pairs):
                if outer_work and k in outer_work:
                    outer_work[k]()
                arrive(k, n, emit)
            sent("e", pa.at[pl.ds(0, 2 * pairs), :, pl.ds(0, n)])

        @pl.when(jnp.logical_not(is_end))
        def _():
            def mine(m):
                return 2 * m + dp - 1

            def other(m):
                return 2 * m + 2 - dp

            def to_mid(k, m):
                return rc(cols(ff, k), cols(ff, k), "f", m, dp=midn)

            def to_end(k):
                return rc(cols(ff, k), cols(ff, k), "h", k, dp=endn)

            def forward_result(m):
                k = other(m)
                rc(cols(ff, k), cols(ff, k), "f", m, dp=midn).wait_recv()
                to_end(k).start()
                emit(k)

            for m in range(ahead):
                pass_on(m, n, p_wait)
            for m in range(pairs):
                if m + ahead < pairs:
                    pass_on(m + ahead, n, p_wait)
                if inner_work and m in inner_work:
                    inner_work[m]()
                k = mine(m)
                p_wait(k)
                e_wait(k, n)
                to_root(m, n).wait_recv()
                ff[k, :, :n] = pa[k, :, :n] + re[k, :, :n] + rm[m, :, :n]
                to_end(k).start()
                to_mid(k, m).start()
                emit(k)
                if m > 0:
                    forward_result(m - 1)
            forward_result(pairs - 1)
            half_of = pl.ds(0, pairs)
            sent("m", tt.at[half_of, :, pl.ds(0, n)])
            sent("f", tt.at[half_of, :, pl.ds(0, n)])
            sent("h", pa.at[pl.ds(0, 2 * pairs), :, pl.ds(0, n)])

    @pl.when(st == 1)
    def _():
        def own_w(k, dst_k):
            return wc.at[:, :, :, lanes(k)], w4.at[:, :, lanes(dst_k)]

        def own_s(k, dst_k):
            return ws.at[:, lanes(k)], s4.at[lanes(dst_k)]

        loads = [local(gz, dzl, 0), local(*own_w(tp, tp), 1), local(*own_s(tp, tp), 2)]
        for c in loads:
            c.start()

        def w_copy(o):
            return rc(*own_w(owner(o), tp), "w", o, tp=owner(o))

        def s_copy(o):
            return rc(*own_s(owner(o), tp), "v", o, tp=owner(o))

        def w_half(o, k, h):
            rows = pl.ds(k * B + h * HB, HB)
            return w4.at[:, :, rows], s4.at[rows]

        def far_copies(o):
            k = owner(o)
            mine = pl.ds(odd * HB, HB)
            dst_w, dst_s = w_half(o, tp, odd)
            return rc(wc.at[:, :, mine, lanes(k)], dst_w, "w", o, tp=k), rc(ws.at[mine, lanes(k)], dst_s, "v", o, tp=k)

        def far_recv(o):
            dst_w, dst_s = w_half(o, owner(o), odd)
            return rc(dst_w, dst_w, "w", o, tp=owner(o)), rc(dst_s, dst_s, "v", o, tp=owner(o))

        def peer_copies(o, h):
            dst_w, dst_s = w_half(o, owner(o), h)
            return rc(dst_w, dst_w, "i", o, dp=peer), rc(dst_s, dst_s, "j", o, dp=peer)

        far = (2, 3)
        w_sends = [*far_copies(2), *far_copies(3), w_copy(1), s_copy(1)]
        for c in w_sends:
            c.start()

        share = pl.ds(odd * HB, HB)
        quarters = [rc(wc.at[i, :, share], w0.at[i, :, tp, share], "a", i, stage=0) for i in range(3)]
        quarters.append(rc(ws.at[share], s0.at[tp, share], "a", 3, stage=0))
        for o in range(IMGS):
            quarters.append(rc(gam, ga.at[tp], "y", 0, stage=0, tp=owner(o)))
            quarters.append(rc(gams, gsa.at[tp], "u", 0, stage=0, tp=owner(o)))
        for c in quarters:
            c.start()

        edge = jnp.zeros((WP, C), BF)
        for o in range(IMGS):
            for r in (0, HW + 1):
                x4[o, r] = edge
                g4[o, r] = edge
        x4[:, :, 24:, :] = jnp.zeros((IMGS, HW + 2, 8, C), BF)
        d4[:, :, 24:, :] = jnp.zeros((IMGS, HW, 8, B), BF)
        for i in NEAR:
            wf[i, :, W3:] = jnp.zeros((C, B), BF)

        loads[0].wait()
        wide[...] = dzl[...].astype(F32)

        def split_rows(h, c):
            for o in range(IMGS):
                d4[o, h, :HW, :] = wide[pl.ds(h * HW * IMGS + o, HW, stride=IMGS), :].astype(BF)
            return c

        lax.fori_loop(0, HW, split_rows, 0)

        scale_main = gam[...]
        shift_main = bet[...]
        scale_short = gams[...]

        def rows(img, k):
            return xl.at[img, pl.ds(k * HT, HT)]

        def tail_copy(img, k):
            ref = xl.at[img, pl.ds((NT - 1) * HT + CROSS, HT - CROSS)] if k is None else rows(img, k)
            return rc(ref, ref, "c", NT - 1 if k is None else k, tp=nbx)

        def head_copy(img):
            ref = xl.at[img, pl.ds((NT - 1) * HT, CROSS)]
            return rc(ref, ref, "x", 0, stage=0)

        def each_tail(img, k, act):
            @pl.when(k < NT - 1)
            def _():
                act(tail_copy(img, k))

            @pl.when(k == NT - 1)
            def _():
                act(tail_copy(img, None))

        def land(o, k):
            img = owner(o)
            ref = rows(img, k)
            if o == 0:
                rc(ref, ref, "a", k, stage=0).wait_recv()
                rc(ref, ref, "b", k, tp=sib).start()
                each_tail(img, k, lambda c: c.start())
            elif o == 1:
                rc(ref, ref, "b", k, tp=sib).wait_recv()
            elif o == 2:
                each_tail(img, k, lambda c: c.wait_recv())

                @pl.when(k == NT - 1)
                def _():
                    head_copy(img).wait_recv()

                rc(ref, ref, "d", k, tp=sib).start()
            else:
                rc(ref, ref, "d", k, tp=sib).wait_recv()
            for r in range(HT):
                h = k * HT + r
                x4[img, 1 + h, :HW, :] = xl[img, h]

        def weights():
            for c in loads[1:]:
                c.wait()
            rc(*own_w(sib, sib), "w", 1, tp=sib).wait_recv()
            rc(*own_s(sib, sib), "v", 1, tp=sib).wait_recv()
            for o in far:
                for c in peer_copies(o, 1 - odd):
                    c.wait_recv()
            for i in range(3):
                for j in range(3):
                    wf[i, :, j * B:(j + 1) * B] = w4[i, j]
            wf[MAIN, :, W3:] = s4[...]

        def g_copy(o):
            k = owner(o)
            return rc(dzm.at[k], g0.at[tp], "g", o, stage=0, tp=k)

        def tile(img, t):
            h0 = t * HT
            acc = None
            for i in range(3):
                d = jnp.dot(x4[img, pl.ds(h0 + i, HT)].reshape(M, C), wf[i], preferred_element_type=F32)
                acc = d if acc is None else acc + d
            pre = pltpu.roll(acc[:, :B], 1, 0) + acc[:, B:2 * B] + pltpu.roll(acc[:, 2 * B:W3], M - 1, 0)
            mixed = pre * scale_main + shift_main + acc[:, W3:] * scale_short
            z = jnp.maximum(mixed, 0.0)
            for r in range(HT):
                zf[pl.ds((h0 + r) * HW * IMGS + img, HW, stride=IMGS), :] = z[r * WP:r * WP + HW]
            dz = d4[img, pl.ds(h0, HT)].reshape(M, B).astype(F32)
            dz = jnp.where(mixed > 0.0, dz, 0.0)
            dzm[img, pl.ds(h0, HT)] = dz.astype(BF).reshape(HT, WP, B)[:, :HW, :]
            g = dz * scale_main
            for j, val in enumerate((pltpu.roll(g, M - 1, 0), g, pltpu.roll(g, 1, 0), dz * scale_short)):
                g4[img, pl.ds(1 + h0, HT), :, j * B:(j + 1) * B] = val.astype(BF).reshape(HT, WP, B)

        def weight_grad(i, n, e, done):
            hx = jnp.where(e == 0, 1 - half, half)
            c0 = pl.multiple_of(hx * 2 * B, 2 * B)
            acc = None
            for img in range(IMGS):
                rhs = g4[img, 2 - i:2 - i + HW, :, :n].reshape(HW * WP, n)
                d = jnp.dot(xt[img, pl.ds(c0, 2 * B), :], rhs, preferred_element_type=F32)
                acc = d if acc is None else acc + d
            for h in range(NR):
                for p in range(2):
                    r = p * B + h * R
                    done(e, p, h, 2 * hx + p, acc[r:r + R])

        def arrived(o, k):
            img = owner(o)
            land(o, k)

            def run(t, c):
                tile(img, t)
                return c

            lax.fori_loop(jnp.maximum(k - 1, 0), jnp.where(k == NT - 1, NT, k), run, 0)

            @pl.when(k == NT - 1)
            def _():
                if o < 2:
                    g_copy(o).start()
                xt[img] = x4[img, 1:HW + 1].reshape(HW * WP, C).T

        with jax.named_scope("s1_fwd"):
            for o in far:
                for w in far_recv(o):
                    w.wait_recv()
                for w in peer_copies(o, odd):
                    w.start()
            land(0, 0)
            land(1, 0)

            def step(t, c):
                @pl.when(t == 1)
                def _():
                    weights()

                @pl.when(t < NT)
                def _():
                    for o in (0, 1):
                        arrived(o, t)

                for o in far:
                    arrived(o, t - 1)
                return c

            lax.fori_loop(1, NT + 1, step, 0)

        def part_near(k, q):
            return rc(part.at[k, :, pl.ds(0, W3)], pa.at[k, :, pl.ds(0, W3)], "p", k, tp=q)

        def part_main(k):
            return rc(part.at[NEARS + k], pa.at[k], "q", k, stage=0)

        def near_chunk(e, p, h, idx):
            return 2 * NR * (idx + len(NEAR) * (1 - e)) + 2 * h + lax.rem(p + par, 2)

        def near_done(idx):
            def done(e, p, h, q, val):
                k = near_chunk(e, p, h, idx)

                @pl.when(q == tp)
                def _():
                    pa[k, :, :W3] = val

                @pl.when(q != tp)
                def _():
                    part[k, :, :W3] = val
                    part_near(k, q).start()

            return done

        def main_done(e, p, h, q, val):
            k = 2 * NR * e + 2 * h + p
            part[NEARS + k] = val
            part_main(k).start()

        def far_grad(idx):
            weight_grad(NEAR[idx], W3, 0, near_done(idx))

        def p_wait(k):
            @pl.when(jnp.logical_or(k >= 2 * NR * len(NEAR), lax.rem(k, 2) == 1))
            def _():
                part_near(k, sib).wait_recv()

        with jax.named_scope("s1_dw"):
            weight_grad(NEAR[0], W3, 1, near_done(0))
            send_up(range(0, 2 * NR, 2), W3, p_wait)
            weight_grad(MAIN, C, 0, main_done)
            send_up(range(1, 2 * NR, 2), W3, p_wait)
            weight_grad(MAIN, C, 1, main_done)
            weight_grad(NEAR[1], W3, 1, near_done(1))

            @pl.when(is_end)
            def _():
                far_grad(0)

            send_up(range(2 * NR, 4 * NR), W3, p_wait)

            @pl.when(is_end)
            def _():
                far_grad(1)

        def place(i, src, ref, k, h):
            for j in range(3):
                ob[i, j, h * R:(h + 1) * R, lanes(src)] = ref[k, :, j * B:(j + 1) * B]

        with jax.named_scope("s1_ar"):
            send_up(range(4 * NR, NEARS), W3, p_wait)

            z_copy = local(zb, z_out, 4)

            def rest():
                for o in far:
                    g_copy(o).start()
                zb[...] = zf[...].astype(BF)
                z_copy.start()

            inner_work = {1: lambda: far_grad(0), 3: lambda: far_grad(1), LATE: rest}
            all_reduce(NEARS // 2, W3, p_wait, lambda k: None, {LATE: rest}, inner_work, ahead=3)
        outs = [local(ob.at[i], dw_out.at[i], 5 + i) for i in range(3)]
        with jax.named_scope("s1_out"):
            for idx, i in enumerate(NEAR):
                for o in range(IMGS):
                    for h in range(NR):
                        place(i, owner(o), ff, 2 * NR * (idx + len(NEAR) * (o // 2)) + 2 * h + o % 2, h)
                outs[i].start()
            for h in range(NR):
                for o in range(IMGS):
                    src = owner(o)
                    rc(ff.at[o], fo.at[h, src], "o", o, land=(NR * src + h,), stage=0).wait_recv()
                    place(MAIN, src, fo.at[h], src, h)
                    obs[h * R:(h + 1) * R, lanes(src)] = fo[h, src, :, W3:]
            outs[MAIN].start()
            outs.append(local(obs, ds_out, 8))
            outs[-1].start()

        sent("w", w4.at[:, :, pl.ds(0, 2 * B)])
        sent("v", s4.at[pl.ds(0, 2 * B)])
        sent("i", w4.at[:, :, pl.ds(0, B)])
        sent("j", s4.at[pl.ds(0, B)])
        sent("a", x4.at[0, pl.ds(0, W_ROWS // WP)])
        sent("y", ga)
        sent("u", gsa)
        sent("g", dzm)
        sent("b", xl.at[0])
        sent("c", xl.at[0, pl.ds(0, HW - CROSS)])
        sent("d", xl.at[0])
        sent("q", part.at[pl.ds(0, 4 * NR)])
        sent("p", part.at[pl.ds(0, NEARS - 2 * NR), :, pl.ds(0, W3)])
        for c in (z_copy, *outs):
            c.wait()

    @pl.when(st == 0)
    def _():
        def rows(k):
            return act.at[pl.ds(k * HT, HT)], xl.at[tp, pl.ds(k * HT, HT)]

        head = pl.ds((NT - 1) * HT, CROSS)
        sends = [rc(*rows(k), "a", k, stage=1) for k in range(NT)]
        sends.append(rc(act.at[head], xl.at[tp, head], "x", 0, stage=1, tp=nbx))
        for c in sends:
            c.start()

        def wref(q, k, part):
            rows = pl.ds(part * HB, HB)
            return w0.at[k, :, q, rows] if k < 3 else s0.at[q, rows]

        def direct(k):
            ref = wref(tp, k, odd)
            return rc(ref, ref, "a", k, stage=1)

        def across(k, part):
            ref = wref(tp, k, part)
            return rc(ref, ref, "i", k, dp=peer)

        def hop(name, q, k, second, dst):
            ref = wref(q, k, 1 - odd if second else odd)
            return rc(ref, ref, name, k + NT * second, tp=dst)

        steps = [(k, second) for k in range(NT) for second in (0, 1)]
        with jax.named_scope("s0_relay"):
            for n, (k, second) in enumerate(steps):
                if second:
                    across(k, 1 - odd).wait_recv()
                else:
                    direct(k).wait_recv()
                    across(k, odd).start()
                hop("c", tp, k, second, nbx).start()
                hop("b", tp, k, second, sib).start()
                if n > 1:
                    hop("c", nbx, *steps[n - 2], nbx).wait_recv()
                    hop("d", nbx, *steps[n - 2], sib).start()
            for back in steps[-2:]:
                hop("c", nbx, *back, nbx).wait_recv()
                hop("d", nbx, *back, sib).start()
        edge = jnp.zeros((WP, C), BF)
        gp[0] = edge
        gp[HW + 1] = edge
        gp[:, 24:, :] = jnp.zeros((HW + 2, 8, C), BF)
        gsp[:, 24:, :] = jnp.zeros((HW, 8, C), BF)

        def p_wait(k):
            rc(pa.at[k], pa.at[k], "q", k, stage=1).wait_recv()

        def result(k):
            q = 2 * jnp.where(k < 2 * NR, 1 - half, half) + lax.rem(k, 2)
            h = lax.rem(k, 2 * NR) // 2
            return rc(ff.at[k], fo.at[h, tp], "o", k, land=(NR * tp + h,), stage=1, tp=q)

        with jax.named_scope("s0_ar"):
            send_up(range(4 * NR), C, p_wait, LAG, lambda k: result(k).start())
            all_reduce(2 * NR, C, p_wait, lambda k: result(k).start(), first=4 * NR - LAG)

        with jax.named_scope("s0_wait"):
            for step in steps:
                hop("b", sib, *step, sib).wait_recv()
                hop("d", dia, *step, sib).wait_recv()
            rc(ga, ga, "y", 0, stage=1).wait_recv()
            rc(gsa, gsa, "u", 0, stage=1).wait_recv()
            for o in range(IMGS):
                q = owner(o)
                rc(dzm.at[tp], g0.at[q], "g", o, stage=1, tp=q).wait_recv()

        def build(h, c):
            for q in range(IMGS):
                dz = g0[q, h].astype(F32)
                gp[1 + h, :HW, q * B:(q + 1) * B] = (dz * ga[q]).astype(BF)
                gsp[h, :HW, q * B:(q + 1) * B] = (dz * gsa[q]).astype(BF)
            return c

        contract = (((1,), (1,)), ((), ()))

        def dx_tile(t, c):
            h0 = t * HT
            total = None
            for j in (1, 0, 2):
                d = None
                for i in range(3):
                    lhs = gp[pl.ds(h0 + 2 - i, HT)].reshape(M, C)
                    p = lax.dot_general(lhs, w0[i, j].reshape(C, C), contract, preferred_element_type=F32)
                    d = p if d is None else d + p
                if j == 1:
                    d += lax.dot_general(gsp[pl.ds(h0, HT)].reshape(M, C), s0[...].reshape(C, C), contract, preferred_element_type=F32)
                else:
                    d = pltpu.roll(d, M - 1 if j == 0 else 1, 0)
                total = d if total is None else total + d
            dxb[pl.ds(h0, HT)] = total.astype(BF).reshape(HT, WP, C)[:, :HW, :]
            return c

        with jax.named_scope("s0_dx"):
            lax.fori_loop(0, HW, build, 0)
            lax.fori_loop(0, NT, dx_tile, 0)
        dx_copy = local(dxb, dx_out, 5)
        dx_copy.start()

        sent("a", xl.at[0])
        sent("x", xl.at[0, pl.ds(0, CROSS)])
        sent("i", x4.at[0, pl.ds(0, W_ROWS // WP)])
        for name in "bcd":
            sent(name, x4.at[pl.ds(0, 2), pl.ds(0, W_ROWS // WP)])
        sent("o", ff.at[pl.ds(0, 4 * NR)])
        dx_copy.wait()


def scratch_shapes():
    def v(*shape, dtype=BF):
        return pltpu.VMEM(shape, dtype)

    def f(*shape):
        return pltpu.VMEM(shape, F32)

    n = HW * HW * IMGS
    buffers = [
        v(IMGS, HW, HW, C),
        v(IMGS, HW + 2, WP, C),
        v(IMGS, C, HW * WP),
        v(3, 3, C, B),
        v(C, B),
        v(3, C, C),
        v(n, B),
        f(n, B),
        v(IMGS, HW, WP, B),
        v(IMGS, HW, HW, B),
        f(n, B),
        v(n, B),
        v(IMGS, HW + 2, WP, C),
        f(NEARS + 4 * NR, R, C),
        f(NEARS, R, C),
        f(NEARS, R, C),
        f(NEARS // 2, R, C),
        f(NEARS // 2, R, C),
        f(NEARS, R, C),
        f(NR, IMGS, R, C),
        f(3, 3, B, C),
        f(B, C),
        v(3, 3, IMGS, B, C),
        v(IMGS, B, C),
        f(IMGS, 1, B),
        f(IMGS, 1, B),
        v(IMGS, HW, HW, B),
        v(HW + 2, WP, C),
        v(HW, WP, C),
        v(HW, HW, C),
    ]
    sems = {}
    for names, n in (("yux", 1), ("awvgij", IMGS), ("bcd", 2 * IMGS), ("oq", 4 * NR), ("mf", NEARS // 2), ("ep", NEARS)):
        for name in names:
            sems["s" + name] = 1
            sems["r" + name] = n
    sems["sh"] = 1
    sems["l"] = 9
    return [*buffers, {k: pltpu.SemaphoreType.DMA((n,)) for k, n in sems.items()}]


def place_kernel(z, dx, dw, ds, z_out, dx_out, dw_out, ds_out, zb, dxb, dwb, dsb, sem_in, sem_out):
    st = lax.axis_index("stage")
    zs = (z, zb, z_out)
    xs = (dx, dxb, dx_out)
    ws = (dw, dwb, dw_out)
    ss = (ds, dsb, ds_out)

    def move(moved, zeroed):
        copies = [(pltpu.make_async_copy(a, b, sem_in.at[k]), pltpu.make_async_copy(b, c, sem_out.at[k])) for k, (a, b, c) in enumerate(moved)]
        for load, _ in copies:
            load.start()
        fills = [pltpu.make_async_copy(b, c, sem_out.at[len(moved) + k]) for k, (_, b, c) in enumerate(zeroed)]
        for (_, b, _), c in zip(zeroed, fills):
            b[...] = jnp.zeros_like(b)
            c.start()
        for load, store in copies:
            load.wait()
            store.start()
        for _, store in copies:
            store.wait()
        for c in fills:
            c.wait()

    @pl.when(st == 1)
    def _():
        move([zs, ss, ws], [xs])

    @pl.when(st == 0)
    def _():
        move([xs], [zs, ss, ws])


def solution(mesh):
    act_spec = P("stage", ("dp", "tp"), None, None, None)
    kernel_spec = P("stage", None, None, "tp", None)
    short_spec = P("stage", "tp", None)
    vec_spec = P("stage", "tp")
    grad_spec = P("stage", "dp", None, None, "tp")
    any_ = pl.BlockSpec(memory_space=pl.ANY)
    vm = pl.BlockSpec(memory_space=pltpu.VMEM)

    def device_step(act_in, w_conv, w_short, gamma, beta, gamma_s, grad_z):
        by_pixel = (0, 2, 3, 1, 4)
        grads = jnp.transpose(grad_z, by_pixel).reshape(-1, B)
        call = pl.pallas_call(
            block_kernel,
            out_shape=(
                jax.ShapeDtypeStruct(grads.shape, BF),
                jax.ShapeDtypeStruct(act_in.shape[2:], BF),
                jax.ShapeDtypeStruct(w_conv.shape[1:], F32),
                jax.ShapeDtypeStruct(w_short.shape[1:], F32),
            ),
            in_specs=[any_, any_, any_, vm, vm, vm, any_],
            out_specs=(any_, any_, any_, any_),
            scratch_shapes=scratch_shapes(),
            compiler_params=pltpu.CompilerParams(vmem_limit_bytes=64000000, has_side_effects=True, collective_id=0),
        )
        found = call(act_in[0, 0], w_conv[0], w_short[0], gamma, beta, gamma_s, grads)
        z, dx, dw, ds = pl.pallas_call(
            place_kernel,
            out_shape=tuple(jax.ShapeDtypeStruct(a.shape, a.dtype) for a in found),
            in_specs=[any_] * 4,
            out_specs=(any_,) * 4,
            scratch_shapes=[*(pltpu.VMEM(a.shape, a.dtype) for a in found), pltpu.SemaphoreType.DMA((4,)), pltpu.SemaphoreType.DMA((4,))],
            compiler_params=pltpu.CompilerParams(vmem_limit_bytes=64000000),
        )(*found)
        z = jnp.transpose(z.reshape(1, HW, HW, IMGS, B), (0, 3, 1, 2, 4))
        return z, dx[None, None], dw[None], ds[None]

    return jax.shard_map(device_step, mesh=mesh, in_specs=(act_spec, kernel_spec, short_spec, vec_spec, vec_spec, vec_spec, grad_spec), out_specs=(grad_spec, act_spec, kernel_spec, short_spec), check_vma=False)
```

```python
import jax
import jax.numpy as jnp
from jax import lax
from jax.experimental import pallas as pl
from jax.experimental.pallas import tpu as pltpu
from jax.sharding import PartitionSpec as P

BF = jnp.bfloat16
F32 = jnp.float32
MESH = pl.DeviceIdType.MESH
B = 128
C = 4 * B
W3 = 3 * B
IMGS = 4
HW = 28
WP = 32
HT = 7
NT = 4
M = HT * WP
BIG_VMEM = 56000000
SMALL_VMEM = 12000000
LAG = 12
LATE = 7
R = 32
NR = B // R
W_ROWS = 10 * B // 2
HB = B // 2
CROSS = 4
NEAR = (0, 2)
NEARS = 4 * NR * len(NEAR)
MAIN = 1


def lanes(k):
    return pl.ds(pl.multiple_of(k * B, B), B)


def block_kernel(act, wc, ws, gam, bet, gams, gz, z_out, dx_out, dw_out, ds_out,
                 xl, x4, xt, w4, s4, wf, dzl, wide, d4, dzm, zf, g4, part, pa, re, rm, tt, ff, fo,
                 w0, s0, ga, gsa, g0, gp, gsp, sem):
    dp = lax.axis_index("dp")
    st = lax.axis_index("stage")
    tp = lax.axis_index("tp")
    par = lax.rem(tp, 2)
    half = tp // 2
    sib = tp + 1 - 2 * par
    nbx = lax.rem(tp + 2, IMGS)
    dia = lax.rem(sib + 2, IMGS)
    odd = lax.rem(dp, 2)
    peer = dp + 1 - 2 * odd

    barrier = pltpu.get_barrier_semaphore()

    def greet(**dev):
        pl.semaphore_signal(barrier, inc=1, device_id=dev, device_id_type=MESH)

    for mate in (sib, nbx, dia):
        greet(tp=mate)
        greet(stage=1 - st, tp=mate)
    greet(stage=1 - st)
    is_end = jnp.logical_or(dp == 0, dp == 3)
    inner = jnp.where(dp == 0, 1, 2)
    endn = jnp.where(dp == 1, 0, 3)
    midn = 3 - dp
    mates = 7

    @pl.when(is_end)
    def _():
        greet(dp=inner)
        pl.semaphore_wait(barrier, mates + 1)

    @pl.when(jnp.logical_not(is_end))
    def _():
        greet(dp=endn)
        greet(dp=midn)
        pl.semaphore_wait(barrier, mates + 2)

    def rc(src, dst, name, *k, land=None, **dev):
        ssem, rsem = sem["s" + name], sem["r" + name.replace("h", "e")]
        return pltpu.make_async_remote_copy(src_ref=src, dst_ref=dst, send_sem=ssem.at[0], recv_sem=rsem.at[land or k], device_id=dev, device_id_type=MESH)

    def sent(name, ref):
        pltpu.make_async_remote_copy(src_ref=ref, dst_ref=ref, send_sem=sem["s" + name].at[0], recv_sem=sem["re"].at[0], device_id={"tp": sib}, device_id_type=MESH).wait_send()

    def local(src, dst, k):
        return pltpu.make_async_copy(src, dst, sem["l"].at[k])

    def owner(o):
        return jnp.where(o == 0, tp, jnp.where(o == 1, sib, jnp.where(o == 2, nbx, dia)))

    def up(k, n):
        return rc(pa.at[k, :, pl.ds(0, n)], re.at[k, :, pl.ds(0, n)], "e", k, dp=inner)

    def arrive(k, n, emit):
        ref = ff.at[k, :, pl.ds(0, n)]
        rc(ref, ref, "h", k, dp=inner).wait_recv()
        emit(k)

    def send_up(ks, n, p_wait, lag=None, emit=None):
        @pl.when(is_end)
        def _():
            for k in ks:
                p_wait(k)
                up(k, n).start()
                if lag is not None and k >= lag:
                    arrive(k - lag, n, emit)

    def e_wait(k, n):
        rc(pa.at[k, :, pl.ds(0, n)], re.at[k, :, pl.ds(0, n)], "e", k, dp=endn).wait_recv()

    def to_root(m, n):
        return rc(tt.at[m, :, pl.ds(0, n)], rm.at[m, :, pl.ds(0, n)], "m", m, dp=midn)

    def pass_on(m, n, p_wait):
        k = 2 * m + 2 - dp
        p_wait(k)
        e_wait(k, n)
        tt[m, :, :n] = pa[k, :, :n] + re[k, :, :n]
        to_root(m, n).start()

    def all_reduce(pairs, n, p_wait, emit, outer_work=None, inner_work=None, first=0, ahead=1):
        def cols(ref, k):
            return ref.at[k, :, pl.ds(0, n)]

        @pl.when(is_end)
        def _():
            for k in range(first, 2 * pairs):
                if outer_work and k in outer_work:
                    outer_work[k]()
                arrive(k, n, emit)
            sent("e", pa.at[pl.ds(0, 2 * pairs), :, pl.ds(0, n)])

        @pl.when(jnp.logical_not(is_end))
        def _():
            def mine(m):
                return 2 * m + dp - 1

            def other(m):
                return 2 * m + 2 - dp

            def to_mid(k, m):
                return rc(cols(ff, k), cols(ff, k), "f", m, dp=midn)

            def to_end(k):
                return rc(cols(ff, k), cols(ff, k), "h", k, dp=endn)

            def forward_result(m):
                k = other(m)
                rc(cols(ff, k), cols(ff, k), "f", m, dp=midn).wait_recv()
                to_end(k).start()
                emit(k)

            for m in range(ahead):
                pass_on(m, n, p_wait)
            for m in range(pairs):
                if m + ahead < pairs:
                    pass_on(m + ahead, n, p_wait)
                if inner_work and m in inner_work:
                    inner_work[m]()
                k = mine(m)
                p_wait(k)
                e_wait(k, n)
                to_root(m, n).wait_recv()
                ff[k, :, :n] = pa[k, :, :n] + re[k, :, :n] + rm[m, :, :n]
                to_end(k).start()
                to_mid(k, m).start()
                emit(k)
                if m > 0:
                    forward_result(m - 1)
            forward_result(pairs - 1)
            half_of = pl.ds(0, pairs)
            sent("m", tt.at[half_of, :, pl.ds(0, n)])
            sent("f", tt.at[half_of, :, pl.ds(0, n)])
            sent("h", pa.at[pl.ds(0, 2 * pairs), :, pl.ds(0, n)])

    @pl.when(st == 1)
    def _():
        def own_w(k, dst_k):
            return wc.at[:, :, :, lanes(k)], w4.at[:, :, lanes(dst_k)]

        def own_s(k, dst_k):
            return ws.at[:, lanes(k)], s4.at[lanes(dst_k)]

        loads = [local(gz, dzl, 0), local(*own_w(tp, tp), 1), local(*own_s(tp, tp), 2)]
        for c in loads:
            c.start()

        def w_copy(o):
            return rc(*own_w(owner(o), tp), "w", o, tp=owner(o))

        def s_copy(o):
            return rc(*own_s(owner(o), tp), "v", o, tp=owner(o))

        def w_half(o, k, h):
            rows = pl.ds(k * B + h * HB, HB)
            return w4.at[:, :, rows], s4.at[rows]

        def far_copies(o):
            k = owner(o)
            mine = pl.ds(odd * HB, HB)
            dst_w, dst_s = w_half(o, tp, odd)
            return rc(wc.at[:, :, mine, lanes(k)], dst_w, "w", o, tp=k), rc(ws.at[mine, lanes(k)], dst_s, "v", o, tp=k)

        def far_recv(o):
            dst_w, dst_s = w_half(o, owner(o), odd)
            return rc(dst_w, dst_w, "w", o, tp=owner(o)), rc(dst_s, dst_s, "v", o, tp=owner(o))

        def peer_copies(o, h):
            dst_w, dst_s = w_half(o, owner(o), h)
            return rc(dst_w, dst_w, "i", o, dp=peer), rc(dst_s, dst_s, "j", o, dp=peer)

        far = (2, 3)
        w_sends = [*far_copies(2), *far_copies(3), w_copy(1), s_copy(1)]
        for c in w_sends:
            c.start()

        share = pl.ds(odd * HB, HB)
        quarters = [rc(wc.at[i, :, share], w0.at[i, :, tp, share], "a", i, stage=0) for i in range(3)]
        quarters.append(rc(ws.at[share], s0.at[tp, share], "a", 3, stage=0))
        for o in range(IMGS):
            quarters.append(rc(gam, ga.at[tp], "y", 0, stage=0, tp=owner(o)))
            quarters.append(rc(gams, gsa.at[tp], "u", 0, stage=0, tp=owner(o)))
        for c in quarters:
            c.start()

        edge = jnp.zeros((WP, C), BF)
        for o in range(IMGS):
            for r in (0, HW + 1):
                x4[o, r] = edge
                g4[o, r] = edge
        x4[:, :, 24:, :] = jnp.zeros((IMGS, HW + 2, 8, C), BF)
        d4[:, :, 24:, :] = jnp.zeros((IMGS, HW, 8, B), BF)
        for i in NEAR:
            wf[i, :, W3:] = jnp.zeros((C, B), BF)

        loads[0].wait()
        wide[...] = dzl[...].astype(F32)

        def split_rows(h, c):
            for o in range(IMGS):
                d4[o, h, :HW, :] = wide[pl.ds(h * HW * IMGS + o, HW, stride=IMGS), :].astype(BF)
            return c

        lax.fori_loop(0, HW, split_rows, 0)

        scale_main = gam[...]
        shift_main = bet[...]
        scale_short = gams[...]

        def rows(img, k):
            return xl.at[img, pl.ds(k * HT, HT)]

        def tail_copy(img, k):
            ref = xl.at[img, pl.ds((NT - 1) * HT + CROSS, HT - CROSS)] if k is None else rows(img, k)
            return rc(ref, ref, "c", NT - 1 if k is None else k, tp=nbx)

        def head_copy(img):
            ref = xl.at[img, pl.ds((NT - 1) * HT, CROSS)]
            return rc(ref, ref, "x", 0, stage=0)

        def each_tail(img, k, act):
            @pl.when(k < NT - 1)
            def _():
                act(tail_copy(img, k))

            @pl.when(k == NT - 1)
            def _():
                act(tail_copy(img, None))

        def land(o, k):
            img = owner(o)
            ref = rows(img, k)
            if o == 0:
                rc(ref, ref, "a", k, stage=0).wait_recv()
                rc(ref, ref, "b", k, tp=sib).start()
                each_tail(img, k, lambda c: c.start())
            elif o == 1:
                rc(ref, ref, "b", k, tp=sib).wait_recv()
            elif o == 2:
                each_tail(img, k, lambda c: c.wait_recv())

                @pl.when(k == NT - 1)
                def _():
                    head_copy(img).wait_recv()

                rc(ref, ref, "d", k, tp=sib).start()
            else:
                rc(ref, ref, "d", k, tp=sib).wait_recv()
            for r in range(HT):
                h = k * HT + r
                x4[img, 1 + h, :HW, :] = xl[img, h]

        def weights():
            for c in loads[1:]:
                c.wait()
            rc(*own_w(sib, sib), "w", 1, tp=sib).wait_recv()
            rc(*own_s(sib, sib), "v", 1, tp=sib).wait_recv()
            for o in far:
                for c in peer_copies(o, 1 - odd):
                    c.wait_recv()
            for i in range(3):
                for j in range(3):
                    wf[i, :, j * B:(j + 1) * B] = w4[i, j]
            wf[MAIN, :, W3:] = s4[...]

        def g_copy(o):
            k = owner(o)
            return rc(dzm.at[k], g0.at[tp], "g", o, stage=0, tp=k)

        def tile(img, t):
            h0 = t * HT
            acc = None
            for i in range(3):
                d = jnp.dot(x4[img, pl.ds(h0 + i, HT)].reshape(M, C), wf[i], preferred_element_type=F32)
                acc = d if acc is None else acc + d
            pre = pltpu.roll(acc[:, :B], 1, 0) + acc[:, B:2 * B] + pltpu.roll(acc[:, 2 * B:W3], M - 1, 0)
            mixed = pre * scale_main + shift_main + acc[:, W3:] * scale_short
            z = jnp.maximum(mixed, 0.0)
            for r in range(HT):
                zf[pl.ds((h0 + r) * HW * IMGS + img, HW, stride=IMGS), :] = z[r * WP:r * WP + HW]
            dz = d4[img, pl.ds(h0, HT)].reshape(M, B).astype(F32)
            dz = jnp.where(mixed > 0.0, dz, 0.0)
            dzm[img, pl.ds(h0, HT)] = dz.astype(BF).reshape(HT, WP, B)[:, :HW, :]
            g = dz * scale_main
            for j, val in enumerate((pltpu.roll(g, M - 1, 0), g, pltpu.roll(g, 1, 0), dz * scale_short)):
                g4[img, pl.ds(1 + h0, HT), :, j * B:(j + 1) * B] = val.astype(BF).reshape(HT, WP, B)

        def weight_grad(i, n, e, done):
            hx = jnp.where(e == 0, 1 - half, half)
            c0 = pl.multiple_of(hx * 2 * B, 2 * B)
            acc = None
            for img in range(IMGS):
                rhs = g4[img, 2 - i:2 - i + HW, :, :n].reshape(HW * WP, n)
                d = jnp.dot(xt[img, pl.ds(c0, 2 * B), :], rhs, preferred_element_type=F32)
                acc = d if acc is None else acc + d
            for h in range(NR):
                for p in range(2):
                    r = p * B + h * R
                    done(e, p, h, 2 * hx + p, acc[r:r + R])

        def arrived(o, k):
            img = owner(o)
            land(o, k)

            def run(t, c):
                tile(img, t)
                if o < 2:
                    some = pl.ds(t * HT, HT)
                    rc(dzm.at[img, some], g0.at[tp, some], "g", o, stage=0, tp=img).start()
                return c

            lax.fori_loop(jnp.maximum(k - 1, 0), jnp.where(k == NT - 1, NT, k), run, 0)

            @pl.when(k == NT - 1)
            def _():
                xt[img] = x4[img, 1:HW + 1].reshape(HW * WP, C).T

        with jax.named_scope("s1_fwd"):
            for o in far:
                for w in far_recv(o):
                    w.wait_recv()
                for w in peer_copies(o, odd):
                    w.start()
            land(0, 0)
            land(1, 0)

            def step(t, c):
                @pl.when(t == 1)
                def _():
                    weights()

                @pl.when(t < NT)
                def _():
                    for o in (0, 1):
                        arrived(o, t)

                for o in far:
                    arrived(o, t - 1)
                return c

            lax.fori_loop(1, NT + 1, step, 0)

        def part_near(k, q):
            return rc(part.at[k, :, pl.ds(0, W3)], pa.at[k, :, pl.ds(0, W3)], "p", k, tp=q)

        def part_main(k):
            return rc(part.at[NEARS + k], pa.at[k], "q", k, stage=0)

        def near_chunk(e, p, h, idx):
            return 2 * NR * (idx + len(NEAR) * (1 - e)) + 2 * h + lax.rem(p + par, 2)

        def near_done(idx):
            def done(e, p, h, q, val):
                k = near_chunk(e, p, h, idx)

                @pl.when(q == tp)
                def _():
                    pa[k, :, :W3] = val

                @pl.when(q != tp)
                def _():
                    part[k, :, :W3] = val
                    part_near(k, q).start()

            return done

        def main_done(e, p, h, q, val):
            k = 2 * NR * e + 2 * h + p
            part[NEARS + k] = val
            part_main(k).start()

        def far_grad(idx):
            weight_grad(NEAR[idx], W3, 0, near_done(idx))

        def p_wait(k):
            @pl.when(jnp.logical_or(k >= 2 * NR * len(NEAR), lax.rem(k, 2) == 1))
            def _():
                part_near(k, sib).wait_recv()

        with jax.named_scope("s1_dw"):
            weight_grad(NEAR[0], W3, 1, near_done(0))
            send_up(range(0, 2 * NR, 2), W3, p_wait)
            weight_grad(MAIN, C, 0, main_done)
            send_up(range(1, 2 * NR, 2), W3, p_wait)
            weight_grad(MAIN, C, 1, main_done)
            weight_grad(NEAR[1], W3, 1, near_done(1))

            @pl.when(is_end)
            def _():
                far_grad(0)

            send_up(range(2 * NR, 4 * NR), W3, p_wait)

            @pl.when(is_end)
            def _():
                far_grad(1)

        def place(i, src, ref, k, h):
            for j in range(3):
                dw_out[i, j, h * R:(h + 1) * R, lanes(src)] = ref[k, :, j * B:(j + 1) * B]

        with jax.named_scope("s1_ar"):
            send_up(range(4 * NR, NEARS), W3, p_wait)

            def rest():
                for o in far:
                    g_copy(o).start()
                z_out[...] = zf[...].astype(BF)

            inner_work = {1: lambda: far_grad(0), 3: lambda: far_grad(1), LATE: rest}
            all_reduce(NEARS // 2, W3, p_wait, lambda k: None, {LATE: rest}, inner_work, ahead=2)
        with jax.named_scope("s1_out"):
            for idx, i in enumerate(NEAR):
                for o in range(IMGS):
                    for h in range(NR):
                        place(i, owner(o), ff, 2 * NR * (idx + len(NEAR) * (o // 2)) + 2 * h + o % 2, h)
            for h in range(NR):
                for o in range(IMGS):
                    src = owner(o)
                    rc(ff.at[o], fo.at[h, src], "o", o, land=(NR * src + h,), stage=0).wait_recv()
                    place(MAIN, src, fo.at[h], src, h)
                    ds_out[h * R:(h + 1) * R, lanes(src)] = fo[h, src, :, W3:]

        sent("w", w4.at[:, :, pl.ds(0, 2 * B)])
        sent("v", s4.at[pl.ds(0, 2 * B)])
        sent("i", w4.at[:, :, pl.ds(0, B)])
        sent("j", s4.at[pl.ds(0, B)])
        sent("a", x4.at[0, pl.ds(0, W_ROWS // WP)])
        sent("y", ga)
        sent("u", gsa)
        sent("g", dzm)
        sent("b", xl.at[0])
        sent("c", xl.at[0, pl.ds(0, HW - CROSS)])
        sent("d", xl.at[0])
        sent("q", part.at[pl.ds(0, 4 * NR)])
        sent("p", part.at[pl.ds(0, NEARS - 2 * NR), :, pl.ds(0, W3)])

    @pl.when(st == 0)
    def _():
        def rows(k):
            return act.at[pl.ds(k * HT, HT)], xl.at[tp, pl.ds(k * HT, HT)]

        head = pl.ds((NT - 1) * HT, CROSS)
        sends = [rc(*rows(k), "a", k, stage=1) for k in range(NT)]
        sends.append(rc(act.at[head], xl.at[tp, head], "x", 0, stage=1, tp=nbx))
        for c in sends:
            c.start()

        def wref(q, k, part):
            rows = pl.ds(part * HB, HB)
            return w0.at[k, :, q, rows] if k < 3 else s0.at[q, rows]

        def direct(k):
            ref = wref(tp, k, odd)
            return rc(ref, ref, "a", k, stage=1)

        def across(k, part):
            ref = wref(tp, k, part)
            return rc(ref, ref, "i", k, dp=peer)

        def hop(name, q, k, second, dst):
            ref = wref(q, k, 1 - odd if second else odd)
            return rc(ref, ref, name, k + NT * second, tp=dst)

        steps = [(k, second) for k in range(NT) for second in (0, 1)]
        with jax.named_scope("s0_relay"):
            for n, (k, second) in enumerate(steps):
                if second:
                    across(k, 1 - odd).wait_recv()
                else:
                    direct(k).wait_recv()
                    across(k, odd).start()
                hop("c", tp, k, second, nbx).start()
                hop("b", tp, k, second, sib).start()
                if n > 1:
                    hop("c", nbx, *steps[n - 2], nbx).wait_recv()
                    hop("d", nbx, *steps[n - 2], sib).start()
            for back in steps[-2:]:
                hop("c", nbx, *back, nbx).wait_recv()
                hop("d", nbx, *back, sib).start()
        edge = jnp.zeros((WP, C), BF)
        gp[0] = edge
        gp[HW + 1] = edge
        gp[:, 24:, :] = jnp.zeros((HW + 2, 8, C), BF)
        gsp[:, 24:, :] = jnp.zeros((HW, 8, C), BF)

        def p_wait(k):
            rc(pa.at[k], pa.at[k], "q", k, stage=1).wait_recv()

        def result(k):
            q = 2 * jnp.where(k < 2 * NR, 1 - half, half) + lax.rem(k, 2)
            h = lax.rem(k, 2 * NR) // 2
            return rc(ff.at[k], fo.at[h, tp], "o", k, land=(NR * tp + h,), stage=1, tp=q)

        with jax.named_scope("s0_ar"):
            send_up(range(4 * NR), C, p_wait, LAG, lambda k: result(k).start())
            all_reduce(2 * NR, C, p_wait, lambda k: result(k).start(), first=4 * NR - LAG)

        with jax.named_scope("s0_wait"):
            for step in steps:
                hop("b", sib, *step, sib).wait_recv()
                hop("d", dia, *step, sib).wait_recv()
            rc(ga, ga, "y", 0, stage=1).wait_recv()
            rc(gsa, gsa, "u", 0, stage=1).wait_recv()
            for o in range(IMGS):
                q = owner(o)
                rc(dzm.at[tp], g0.at[q], "g", o, stage=1, tp=q).wait_recv()

        def build(h, c):
            for q in range(IMGS):
                dz = g0[q, h].astype(F32)
                gp[1 + h, :HW, q * B:(q + 1) * B] = (dz * ga[q]).astype(BF)
                gsp[h, :HW, q * B:(q + 1) * B] = (dz * gsa[q]).astype(BF)
            return c

        contract = (((1,), (1,)), ((), ()))

        def dx_tile(t, c):
            h0 = t * HT
            total = None
            for j in (1, 0, 2):
                d = None
                for i in range(3):
                    lhs = gp[pl.ds(h0 + 2 - i, HT)].reshape(M, C)
                    p = lax.dot_general(lhs, w0[i, j].reshape(C, C), contract, preferred_element_type=F32)
                    d = p if d is None else d + p
                if j == 1:
                    d += lax.dot_general(gsp[pl.ds(h0, HT)].reshape(M, C), s0[...].reshape(C, C), contract, preferred_element_type=F32)
                else:
                    d = pltpu.roll(d, M - 1 if j == 0 else 1, 0)
                total = d if total is None else total + d
            dx_out[pl.ds(h0, HT)] = total.astype(BF).reshape(HT, WP, C)[:, :HW, :]
            return c

        with jax.named_scope("s0_dx"):
            lax.fori_loop(0, HW, build, 0)
            lax.fori_loop(0, NT, dx_tile, 0)

        sent("a", xl.at[0])
        sent("x", xl.at[0, pl.ds(0, CROSS)])
        sent("i", x4.at[0, pl.ds(0, W_ROWS // WP)])
        for name in "bcd":
            sent(name, x4.at[pl.ds(0, 2), pl.ds(0, W_ROWS // WP)])
        sent("o", ff.at[pl.ds(0, 4 * NR)])


def scratch_shapes():
    def v(*shape, dtype=BF):
        return pltpu.VMEM(shape, dtype)

    def f(*shape):
        return pltpu.VMEM(shape, F32)

    n = HW * HW * IMGS
    buffers = [
        v(IMGS, HW, HW, C),
        v(IMGS, HW + 2, WP, C),
        v(IMGS, C, HW * WP),
        v(3, 3, C, B),
        v(C, B),
        v(3, C, C),
        v(n, B),
        f(n, B),
        v(IMGS, HW, WP, B),
        v(IMGS, HW, HW, B),
        f(n, B),
        v(IMGS, HW + 2, WP, C),
        f(NEARS + 4 * NR, R, C),
        f(NEARS, R, C),
        f(NEARS, R, C),
        f(NEARS // 2, R, C),
        f(NEARS // 2, R, C),
        f(NEARS, R, C),
        f(NR, IMGS, R, C),
        v(3, 3, IMGS, B, C),
        v(IMGS, B, C),
        f(IMGS, 1, B),
        f(IMGS, 1, B),
        v(IMGS, HW, HW, B),
        v(HW + 2, WP, C),
        v(HW, WP, C),
    ]
    sems = {}
    for names, n in (("yux", 1), ("awvgij", IMGS), ("bcd", 2 * IMGS), ("oq", 4 * NR), ("mf", NEARS // 2), ("ep", NEARS)):
        for name in names:
            sems["s" + name] = 1
            sems["r" + name] = n
    sems["sh"] = 1
    sems["l"] = 3
    return [*buffers, {k: pltpu.SemaphoreType.DMA((n,)) for k, n in sems.items()}]


def place_kernel(z, dx, dw, ds, z_out, dx_out, dw_out, ds_out, zb, dxb, dwb, dsb, sem):
    st = lax.axis_index("stage")

    def move(*pairs):
        copies = [pltpu.make_async_copy(a, b, sem.at[k]) for k, (a, b) in enumerate(pairs)]
        for c in copies:
            c.start()
        return copies

    @pl.when(st == 1)
    def _():
        copies = move((dw, dw_out), (ds, ds_out), (z, z_out))
        dxb[...] = jnp.zeros_like(dxb)
        fill = pltpu.make_async_copy(dxb, dx_out, sem.at[3])
        fill.start()
        for c in (*copies, fill):
            c.wait()

    @pl.when(st == 0)
    def _():
        copies = move((dx, dx_out))
        for b in (zb, dwb, dsb):
            b[...] = jnp.zeros_like(b)
        fills = [pltpu.make_async_copy(b, c, sem.at[1 + k]) for k, (b, c) in enumerate(((zb, z_out), (dwb, dw_out), (dsb, ds_out)))]
        for c in fills:
            c.start()
        for c in (*copies, *fills):
            c.wait()


def solution(mesh):
    act_spec = P("stage", ("dp", "tp"), None, None, None)
    kernel_spec = P("stage", None, None, "tp", None)
    short_spec = P("stage", "tp", None)
    vec_spec = P("stage", "tp")
    grad_spec = P("stage", "dp", None, None, "tp")
    any_ = pl.BlockSpec(memory_space=pl.ANY)
    vm = pl.BlockSpec(memory_space=pltpu.VMEM)

    def device_step(act_in, w_conv, w_short, gamma, beta, gamma_s, grad_z):
        by_pixel = (0, 2, 3, 1, 4)
        grads = jnp.transpose(grad_z, by_pixel).reshape(-1, B)
        call = pl.pallas_call(
            block_kernel,
            out_shape=(
                pltpu.VMEM(grads.shape, BF),
                pltpu.VMEM(act_in.shape[2:], BF),
                pltpu.VMEM(w_conv.shape[1:], F32),
                pltpu.VMEM(w_short.shape[1:], F32),
            ),
            in_specs=[any_, any_, any_, vm, vm, vm, any_],
            out_specs=(vm,) * 4,
            scratch_shapes=scratch_shapes(),
            compiler_params=pltpu.CompilerParams(vmem_limit_bytes=BIG_VMEM, has_side_effects=True, collective_id=0),
        )
        found = call(act_in[0, 0], w_conv[0], w_short[0], gamma, beta, gamma_s, grads)
        z, dx, dw, ds = pl.pallas_call(
            place_kernel,
            out_shape=tuple(jax.ShapeDtypeStruct(a.shape, a.dtype) for a in found),
            in_specs=[vm] * 4,
            out_specs=(any_,) * 4,
            scratch_shapes=[*(pltpu.VMEM(a.shape, a.dtype) for a in found), pltpu.SemaphoreType.DMA((4,))],
            compiler_params=pltpu.CompilerParams(vmem_limit_bytes=SMALL_VMEM),
        )(*found)
        z = jnp.transpose(z.reshape(1, HW, HW, IMGS, B), (0, 3, 1, 2, 4))
        return z, dx[None, None], dw[None], ds[None]

    return jax.shard_map(device_step, mesh=mesh, in_specs=(act_spec, kernel_spec, short_spec, vec_spec, vec_spec, vec_spec, grad_spec), out_specs=(grad_spec, act_spec, kernel_spec, short_spec), check_vma=False)
```

```python
import jax
import jax.numpy as jnp
from jax import lax
from jax.experimental import pallas as pl
from jax.experimental.pallas import tpu as pltpu
from jax.sharding import PartitionSpec as P

BF = jnp.bfloat16
F32 = jnp.float32
MESH = pl.DeviceIdType.MESH
B = 128
C = 4 * B
W3 = 3 * B
IMGS = 4
HW = 28
WP = 32
HT = 7
NT = 4
M = HT * WP
BIG_VMEM = 56000000
SMALL_VMEM = 12000000
LAG = 12
LATE = 7
R = 32
NR = B // R
W_ROWS = 10 * B // 2
HB = B // 2
CROSS = 4
NEAR = (0, 2)
NEARS = 4 * NR * len(NEAR)
MAIN = 1


def lanes(k):
    return pl.ds(pl.multiple_of(k * B, B), B)


def block_kernel(act, wc, ws, gam, bet, gams, gz, z_out, dx_out, dw_out, ds_out,
                 xl, x4, xt, w4, s4, wf, dzl, wide, d4, dzm, zf, g4, part, pa, re, rm, tt, ff, fo,
                 w0, s0, ga, gsa, g0, gp, gsp, sem):
    dp = lax.axis_index("dp")
    st = lax.axis_index("stage")
    tp = lax.axis_index("tp")
    par = lax.rem(tp, 2)
    half = tp // 2
    sib = tp + 1 - 2 * par
    nbx = lax.rem(tp + 2, IMGS)
    dia = lax.rem(sib + 2, IMGS)
    odd = lax.rem(dp, 2)
    peer = dp + 1 - 2 * odd

    barrier = pltpu.get_barrier_semaphore()

    def greet(**dev):
        pl.semaphore_signal(barrier, inc=1, device_id=dev, device_id_type=MESH)

    for mate in (sib, nbx, dia):
        greet(tp=mate)
        greet(stage=1 - st, tp=mate)
    greet(stage=1 - st)
    is_end = jnp.logical_or(dp == 0, dp == 3)
    inner = jnp.where(dp == 0, 1, 2)
    endn = jnp.where(dp == 1, 0, 3)
    midn = 3 - dp
    mates = 7

    @pl.when(is_end)
    def _():
        greet(dp=inner)
        pl.semaphore_wait(barrier, mates + 1)

    @pl.when(jnp.logical_not(is_end))
    def _():
        greet(dp=endn)
        greet(dp=midn)
        pl.semaphore_wait(barrier, mates + 2)

    def rc(src, dst, name, *k, land=None, **dev):
        ssem, rsem = sem["s" + name], sem["r" + name.replace("h", "e")]
        return pltpu.make_async_remote_copy(src_ref=src, dst_ref=dst, send_sem=ssem.at[0], recv_sem=rsem.at[land or k], device_id=dev, device_id_type=MESH)

    def sent(name, ref):
        pltpu.make_async_remote_copy(src_ref=ref, dst_ref=ref, send_sem=sem["s" + name].at[0], recv_sem=sem["re"].at[0], device_id={"tp": sib}, device_id_type=MESH).wait_send()

    def local(src, dst, k):
        return pltpu.make_async_copy(src, dst, sem["l"].at[k])

    def owner(o):
        return jnp.where(o == 0, tp, jnp.where(o == 1, sib, jnp.where(o == 2, nbx, dia)))

    def up(k, n):
        return rc(pa.at[k, :, pl.ds(0, n)], re.at[k, :, pl.ds(0, n)], "e", k, dp=inner)

    def arrive(k, n, emit):
        ref = ff.at[k, :, pl.ds(0, n)]
        rc(ref, ref, "h", k, dp=inner).wait_recv()
        emit(k)

    def send_up(ks, n, p_wait, lag=None, emit=None):
        @pl.when(is_end)
        def _():
            for k in ks:
                p_wait(k)
                up(k, n).start()
                if lag is not None and k >= lag:
                    arrive(k - lag, n, emit)

    def e_wait(k, n):
        rc(pa.at[k, :, pl.ds(0, n)], re.at[k, :, pl.ds(0, n)], "e", k, dp=endn).wait_recv()

    def to_root(m, n):
        return rc(tt.at[m, :, pl.ds(0, n)], rm.at[m, :, pl.ds(0, n)], "m", m, dp=midn)

    def pass_on(m, n, p_wait):
        k = 2 * m + 2 - dp
        p_wait(k)
        e_wait(k, n)
        tt[m, :, :n] = pa[k, :, :n] + re[k, :, :n]
        to_root(m, n).start()

    def all_reduce(pairs, n, p_wait, emit, outer_work=None, inner_work=None, first=0, ahead=1):
        def cols(ref, k):
            return ref.at[k, :, pl.ds(0, n)]

        @pl.when(is_end)
        def _():
            for k in range(first, 2 * pairs):
                if outer_work and k in outer_work:
                    outer_work[k]()
                arrive(k, n, emit)
            sent("e", pa.at[pl.ds(0, 2 * pairs), :, pl.ds(0, n)])

        @pl.when(jnp.logical_not(is_end))
        def _():
            def mine(m):
                return 2 * m + dp - 1

            def other(m):
                return 2 * m + 2 - dp

            def to_mid(k, m):
                return rc(cols(ff, k), cols(ff, k), "f", m, dp=midn)

            def to_end(k):
                return rc(cols(ff, k), cols(ff, k), "h", k, dp=endn)

            def forward_result(m):
                k = other(m)
                rc(cols(ff, k), cols(ff, k), "f", m, dp=midn).wait_recv()
                to_end(k).start()
                emit(k)

            for m in range(ahead):
                pass_on(m, n, p_wait)
            for m in range(pairs):
                if m + ahead < pairs:
                    pass_on(m + ahead, n, p_wait)
                if inner_work and m in inner_work:
                    inner_work[m]()
                k = mine(m)
                p_wait(k)
                e_wait(k, n)
                to_root(m, n).wait_recv()
                ff[k, :, :n] = pa[k, :, :n] + re[k, :, :n] + rm[m, :, :n]
                to_end(k).start()
                to_mid(k, m).start()
                emit(k)
                if m > 0:
                    forward_result(m - 1)
            forward_result(pairs - 1)
            half_of = pl.ds(0, pairs)
            sent("m", tt.at[half_of, :, pl.ds(0, n)])
            sent("f", tt.at[half_of, :, pl.ds(0, n)])
            sent("h", pa.at[pl.ds(0, 2 * pairs), :, pl.ds(0, n)])

    @pl.when(st == 1)
    def _():
        def own_w(k, dst_k):
            return wc.at[:, :, :, lanes(k)], w4.at[:, :, lanes(dst_k)]

        def own_s(k, dst_k):
            return ws.at[:, lanes(k)], s4.at[lanes(dst_k)]

        loads = [local(gz, dzl, 0), local(*own_w(tp, tp), 1), local(*own_s(tp, tp), 2)]
        for c in loads:
            c.start()

        def w_copy(o):
            return rc(*own_w(owner(o), tp), "w", o, tp=owner(o))

        def s_copy(o):
            return rc(*own_s(owner(o), tp), "v", o, tp=owner(o))

        def w_half(o, k, h):
            rows = pl.ds(k * B + h * HB, HB)
            return w4.at[:, :, rows], s4.at[rows]

        def far_copies(o):
            k = owner(o)
            mine = pl.ds(odd * HB, HB)
            dst_w, dst_s = w_half(o, tp, odd)
            return rc(wc.at[:, :, mine, lanes(k)], dst_w, "w", o, tp=k), rc(ws.at[mine, lanes(k)], dst_s, "v", o, tp=k)

        def far_recv(o):
            dst_w, dst_s = w_half(o, owner(o), odd)
            return rc(dst_w, dst_w, "w", o, tp=owner(o)), rc(dst_s, dst_s, "v", o, tp=owner(o))

        def peer_copies(o, h):
            dst_w, dst_s = w_half(o, owner(o), h)
            return rc(dst_w, dst_w, "i", o, dp=peer), rc(dst_s, dst_s, "j", o, dp=peer)

        far = (2, 3)
        w_sends = [*far_copies(2), *far_copies(3), w_copy(1), s_copy(1)]
        for c in w_sends:
            c.start()

        share = pl.ds(odd * HB, HB)
        quarters = [rc(wc.at[i, :, share], w0.at[i, :, tp, share], "a", i, stage=0) for i in range(3)]
        quarters.append(rc(ws.at[share], s0.at[tp, share], "a", 3, stage=0))
        for o in range(IMGS):
            quarters.append(rc(gam, ga.at[tp], "y", 0, stage=0, tp=owner(o)))
            quarters.append(rc(gams, gsa.at[tp], "u", 0, stage=0, tp=owner(o)))
        for c in quarters:
            c.start()

        edge = jnp.zeros((WP, C), BF)
        for o in range(IMGS):
            for r in (0, HW + 1):
                x4[o, r] = edge
                g4[o, r] = edge
        x4[:, :, 24:, :] = jnp.zeros((IMGS, HW + 2, 8, C), BF)
        d4[:, :, 24:, :] = jnp.zeros((IMGS, HW, 8, B), BF)
        for i in NEAR:
            wf[i, :, W3:] = jnp.zeros((C, B), BF)

        loads[0].wait()
        wide[...] = dzl[...].astype(F32)

        def split_rows(h, c):
            for o in range(IMGS):
                d4[o, h, :HW, :] = wide[pl.ds(h * HW * IMGS + o, HW, stride=IMGS), :].astype(BF)
            return c

        lax.fori_loop(0, HW, split_rows, 0)

        scale_main = gam[...]
        shift_main = bet[...]
        scale_short = gams[...]

        def rows(img, k):
            return xl.at[img, pl.ds(k * HT, HT)]

        def tail_copy(img, k):
            ref = xl.at[img, pl.ds((NT - 1) * HT + CROSS, HT - CROSS)] if k is None else rows(img, k)
            return rc(ref, ref, "c", NT - 1 if k is None else k, tp=nbx)

        def head_copy(img):
            ref = xl.at[img, pl.ds((NT - 1) * HT, CROSS)]
            return rc(ref, ref, "x", 0, stage=0)

        def each_tail(img, k, act):
            @pl.when(k < NT - 1)
            def _():
                act(tail_copy(img, k))

            @pl.when(k == NT - 1)
            def _():
                act(tail_copy(img, None))

        def land(o, k):
            img = owner(o)
            ref = rows(img, k)
            if o == 0:
                rc(ref, ref, "a", k, stage=0).wait_recv()
                rc(ref, ref, "b", k, tp=sib).start()
                each_tail(img, k, lambda c: c.start())
            elif o == 1:
                rc(ref, ref, "b", k, tp=sib).wait_recv()
            elif o == 2:
                each_tail(img, k, lambda c: c.wait_recv())

                @pl.when(k == NT - 1)
                def _():
                    head_copy(img).wait_recv()

                rc(ref, ref, "d", k, tp=sib).start()
            else:
                rc(ref, ref, "d", k, tp=sib).wait_recv()
            for r in range(HT):
                h = k * HT + r
                x4[img, 1 + h, :HW, :] = xl[img, h]

        def weights():
            for c in loads[1:]:
                c.wait()
            rc(*own_w(sib, sib), "w", 1, tp=sib).wait_recv()
            rc(*own_s(sib, sib), "v", 1, tp=sib).wait_recv()
            for o in far:
                for c in peer_copies(o, 1 - odd):
                    c.wait_recv()
            for i in range(3):
                for j in range(3):
                    wf[i, :, j * B:(j + 1) * B] = w4[i, j]
            wf[MAIN, :, W3:] = s4[...]

        def g_copy(o):
            k = owner(o)
            return rc(dzm.at[k], g0.at[tp], "g", o, stage=0, tp=k)

        def tile(img, t):
            h0 = t * HT
            acc = None
            for i in range(3):
                d = jnp.dot(x4[img, pl.ds(h0 + i, HT)].reshape(M, C), wf[i], preferred_element_type=F32)
                acc = d if acc is None else acc + d
            pre = pltpu.roll(acc[:, :B], 1, 0) + acc[:, B:2 * B] + pltpu.roll(acc[:, 2 * B:W3], M - 1, 0)
            mixed = pre * scale_main + shift_main + acc[:, W3:] * scale_short
            z = jnp.maximum(mixed, 0.0)
            for r in range(HT):
                zf[pl.ds((h0 + r) * HW * IMGS + img, HW, stride=IMGS), :] = z[r * WP:r * WP + HW]
            dz = d4[img, pl.ds(h0, HT)].reshape(M, B).astype(F32)
            dz = jnp.where(mixed > 0.0, dz, 0.0)
            dzm[img, pl.ds(h0, HT)] = dz.astype(BF).reshape(HT, WP, B)[:, :HW, :]
            g = dz * scale_main
            for j, val in enumerate((pltpu.roll(g, M - 1, 0), g, pltpu.roll(g, 1, 0), dz * scale_short)):
                g4[img, pl.ds(1 + h0, HT), :, j * B:(j + 1) * B] = val.astype(BF).reshape(HT, WP, B)

        def weight_grad(i, n, e, done):
            hx = jnp.where(e == 0, 1 - half, half)
            c0 = pl.multiple_of(hx * 2 * B, 2 * B)
            acc = None
            for img in range(IMGS):
                rhs = g4[img, 2 - i:2 - i + HW, :, :n].reshape(HW * WP, n)
                d = jnp.dot(xt[img, pl.ds(c0, 2 * B), :], rhs, preferred_element_type=F32)
                acc = d if acc is None else acc + d
            for h in range(NR):
                for p in range(2):
                    r = p * B + h * R
                    done(e, p, h, 2 * hx + p, acc[r:r + R])

        def arrived(o, k):
            img = owner(o)
            land(o, k)

            def run(t, c):
                tile(img, t)
                if o < 2:
                    some = pl.ds(t * HT, HT)
                    rc(dzm.at[img, some], g0.at[tp, some], "g", o, stage=0, tp=img).start()
                return c

            lax.fori_loop(jnp.maximum(k - 1, 0), jnp.where(k == NT - 1, NT, k), run, 0)

            @pl.when(k == NT - 1)
            def _():
                xt[img] = x4[img, 1:HW + 1].reshape(HW * WP, C).T

        with jax.named_scope("s1_fwd"):
            for o in far:
                for w in far_recv(o):
                    w.wait_recv()
                for w in peer_copies(o, odd):
                    w.start()
            land(0, 0)
            land(1, 0)

            def step(t, c):
                @pl.when(t == 1)
                def _():
                    weights()

                @pl.when(t < NT)
                def _():
                    for o in (0, 1):
                        arrived(o, t)

                for o in far:
                    arrived(o, t - 1)
                return c

            lax.fori_loop(1, NT + 1, step, 0)

        def part_near(k, q):
            return rc(part.at[k, :, pl.ds(0, W3)], pa.at[k, :, pl.ds(0, W3)], "p", k, tp=q)

        def part_main(k):
            return rc(part.at[NEARS + k], pa.at[k], "q", k, stage=0)

        def near_chunk(e, p, h, idx):
            return 2 * NR * (idx + len(NEAR) * (1 - e)) + 2 * h + lax.rem(p + par, 2)

        def near_done(idx):
            def done(e, p, h, q, val):
                k = near_chunk(e, p, h, idx)

                @pl.when(q == tp)
                def _():
                    pa[k, :, :W3] = val

                @pl.when(q != tp)
                def _():
                    part[k, :, :W3] = val
                    part_near(k, q).start()

            return done

        def main_done(e, p, h, q, val):
            k = 2 * NR * e + 2 * h + p
            part[NEARS + k] = val
            part_main(k).start()

        def far_grad(idx):
            weight_grad(NEAR[idx], W3, 0, near_done(idx))

        def p_wait(k):
            @pl.when(jnp.logical_or(k >= 2 * NR * len(NEAR), lax.rem(k, 2) == 1))
            def _():
                part_near(k, sib).wait_recv()

        with jax.named_scope("s1_dw"):
            weight_grad(NEAR[0], W3, 1, near_done(0))
            send_up(range(0, 2 * NR, 2), W3, p_wait)
            weight_grad(MAIN, C, 0, main_done)
            send_up(range(1, 2 * NR, 2), W3, p_wait)
            weight_grad(MAIN, C, 1, main_done)
            weight_grad(NEAR[1], W3, 1, near_done(1))

            @pl.when(is_end)
            def _():
                far_grad(0)

            send_up(range(2 * NR, 4 * NR), W3, p_wait)

            @pl.when(is_end)
            def _():
                far_grad(1)

        def place(i, src, ref, k, h):
            for j in range(3):
                dw_out[i, j, h * R:(h + 1) * R, lanes(src)] = ref[k, :, j * B:(j + 1) * B]

        with jax.named_scope("s1_ar"):
            send_up(range(4 * NR, NEARS), W3, p_wait)

            def rest():
                for o in far:
                    g_copy(o).start()
                z_out[...] = zf[...].astype(BF)

            inner_work = {3: lambda: far_grad(0), 5: lambda: far_grad(1), LATE: rest}
            all_reduce(NEARS // 2, W3, p_wait, lambda k: None, {LATE: rest}, inner_work, ahead=2)
        with jax.named_scope("s1_out"):
            for idx, i in enumerate(NEAR):
                for o in range(IMGS):
                    for h in range(NR):
                        place(i, owner(o), ff, 2 * NR * (idx + len(NEAR) * (o // 2)) + 2 * h + o % 2, h)
            for h in range(NR):
                for o in range(IMGS):
                    src = owner(o)
                    rc(ff.at[o], fo.at[h, src], "o", o, land=(NR * src + h,), stage=0).wait_recv()
                    place(MAIN, src, fo.at[h], src, h)
                    ds_out[h * R:(h + 1) * R, lanes(src)] = fo[h, src, :, W3:]

        sent("w", w4.at[:, :, pl.ds(0, 2 * B)])
        sent("v", s4.at[pl.ds(0, 2 * B)])
        sent("i", w4.at[:, :, pl.ds(0, B)])
        sent("j", s4.at[pl.ds(0, B)])
        sent("a", x4.at[0, pl.ds(0, W_ROWS // WP)])
        sent("y", ga)
        sent("u", gsa)
        sent("g", dzm)
        sent("b", xl.at[0])
        sent("c", xl.at[0, pl.ds(0, HW - CROSS)])
        sent("d", xl.at[0])
        sent("q", part.at[pl.ds(0, 4 * NR)])
        sent("p", part.at[pl.ds(0, NEARS - 2 * NR), :, pl.ds(0, W3)])

    @pl.when(st == 0)
    def _():
        def rows(k):
            return act.at[pl.ds(k * HT, HT)], xl.at[tp, pl.ds(k * HT, HT)]

        head = pl.ds((NT - 1) * HT, CROSS)
        sends = [rc(*rows(k), "a", k, stage=1) for k in range(NT)]
        sends.append(rc(act.at[head], xl.at[tp, head], "x", 0, stage=1, tp=nbx))
        for c in sends:
            c.start()

        def wref(q, k, part):
            rows = pl.ds(part * HB, HB)
            return w0.at[k, :, q, rows] if k < 3 else s0.at[q, rows]

        def direct(k):
            ref = wref(tp, k, odd)
            return rc(ref, ref, "a", k, stage=1)

        def across(k, part):
            ref = wref(tp, k, part)
            return rc(ref, ref, "i", k, dp=peer)

        def hop(name, q, k, second, dst):
            ref = wref(q, k, 1 - odd if second else odd)
            return rc(ref, ref, name, k + NT * second, tp=dst)

        steps = [(k, second) for k in range(NT) for second in (0, 1)]
        with jax.named_scope("s0_relay"):
            for n, (k, second) in enumerate(steps):
                if second:
                    across(k, 1 - odd).wait_recv()
                else:
                    direct(k).wait_recv()
                    across(k, odd).start()
                hop("c", tp, k, second, nbx).start()
                hop("b", tp, k, second, sib).start()
                if n > 1:
                    hop("c", nbx, *steps[n - 2], nbx).wait_recv()
                    hop("d", nbx, *steps[n - 2], sib).start()
            for back in steps[-2:]:
                hop("c", nbx, *back, nbx).wait_recv()
                hop("d", nbx, *back, sib).start()
        edge = jnp.zeros((WP, C), BF)
        gp[0] = edge
        gp[HW + 1] = edge
        gp[:, 24:, :] = jnp.zeros((HW + 2, 8, C), BF)
        gsp[:, 24:, :] = jnp.zeros((HW, 8, C), BF)

        def p_wait(k):
            rc(pa.at[k], pa.at[k], "q", k, stage=1).wait_recv()

        def result(k):
            q = 2 * jnp.where(k < 2 * NR, 1 - half, half) + lax.rem(k, 2)
            h = lax.rem(k, 2 * NR) // 2
            return rc(ff.at[k], fo.at[h, tp], "o", k, land=(NR * tp + h,), stage=1, tp=q)

        with jax.named_scope("s0_ar"):
            send_up(range(4 * NR), C, p_wait, LAG, lambda k: result(k).start())
            all_reduce(2 * NR, C, p_wait, lambda k: result(k).start(), first=4 * NR - LAG)

        with jax.named_scope("s0_wait"):
            for step in steps:
                hop("b", sib, *step, sib).wait_recv()
                hop("d", dia, *step, sib).wait_recv()
            rc(ga, ga, "y", 0, stage=1).wait_recv()
            rc(gsa, gsa, "u", 0, stage=1).wait_recv()
            for o in range(IMGS):
                q = owner(o)
                rc(dzm.at[tp], g0.at[q], "g", o, stage=1, tp=q).wait_recv()

        def build(h, c):
            for q in range(IMGS):
                dz = g0[q, h].astype(F32)
                gp[1 + h, :HW, q * B:(q + 1) * B] = (dz * ga[q]).astype(BF)
                gsp[h, :HW, q * B:(q + 1) * B] = (dz * gsa[q]).astype(BF)
            return c

        contract = (((1,), (1,)), ((), ()))

        def dx_tile(t, c):
            h0 = t * 2 * HT
            total = None
            for j in (1, 0, 2):
                d = None
                for i in range(3):
                    lhs = gp[pl.ds(h0 + 2 - i, 2 * HT)].reshape(2 * M, C)
                    p = lax.dot_general(lhs, w0[i, j].reshape(C, C), contract, preferred_element_type=F32)
                    d = p if d is None else d + p
                if j == 1:
                    d += lax.dot_general(gsp[pl.ds(h0, 2 * HT)].reshape(2 * M, C), s0[...].reshape(C, C), contract, preferred_element_type=F32)
                else:
                    d = pltpu.roll(d, 2 * M - 1 if j == 0 else 1, 0)
                total = d if total is None else total + d
            dx_out[pl.ds(h0, 2 * HT)] = total.astype(BF).reshape(2 * HT, WP, C)[:, :HW, :]
            return c

        with jax.named_scope("s0_dx"):
            lax.fori_loop(0, HW, build, 0)
            lax.fori_loop(0, NT // 2, dx_tile, 0)

        sent("a", xl.at[0])
        sent("x", xl.at[0, pl.ds(0, CROSS)])
        sent("i", x4.at[0, pl.ds(0, W_ROWS // WP)])
        for name in "bcd":
            sent(name, x4.at[pl.ds(0, 2), pl.ds(0, W_ROWS // WP)])
        sent("o", ff.at[pl.ds(0, 4 * NR)])


def scratch_shapes():
    def v(*shape, dtype=BF):
        return pltpu.VMEM(shape, dtype)

    def f(*shape):
        return pltpu.VMEM(shape, F32)

    n = HW * HW * IMGS
    buffers = [
        v(IMGS, HW, HW, C),
        v(IMGS, HW + 2, WP, C),
        v(IMGS, C, HW * WP),
        v(3, 3, C, B),
        v(C, B),
        v(3, C, C),
        v(n, B),
        f(n, B),
        v(IMGS, HW, WP, B),
        v(IMGS, HW, HW, B),
        f(n, B),
        v(IMGS, HW + 2, WP, C),
        f(NEARS + 4 * NR, R, C),
        f(NEARS, R, C),
        f(NEARS, R, C),
        f(NEARS // 2, R, C),
        f(NEARS // 2, R, C),
        f(NEARS, R, C),
        f(NR, IMGS, R, C),
        v(3, 3, IMGS, B, C),
        v(IMGS, B, C),
        f(IMGS, 1, B),
        f(IMGS, 1, B),
        v(IMGS, HW, HW, B),
        v(HW + 2, WP, C),
        v(HW, WP, C),
    ]
    sems = {}
    for names, n in (("yux", 1), ("awvgij", IMGS), ("bcd", 2 * IMGS), ("oq", 4 * NR), ("mf", NEARS // 2), ("ep", NEARS)):
        for name in names:
            sems["s" + name] = 1
            sems["r" + name] = n
    sems["sh"] = 1
    sems["l"] = 3
    return [*buffers, {k: pltpu.SemaphoreType.DMA((n,)) for k, n in sems.items()}]


def place_kernel(z, dx, dw, ds, z_out, dx_out, dw_out, ds_out, zb, dxb, dwb, dsb, sem):
    st = lax.axis_index("stage")

    def move(*pairs):
        copies = [pltpu.make_async_copy(a, b, sem.at[k]) for k, (a, b) in enumerate(pairs)]
        for c in copies:
            c.start()
        return copies

    @pl.when(st == 1)
    def _():
        copies = move((dw, dw_out), (ds, ds_out), (z, z_out))
        dxb[...] = jnp.zeros_like(dxb)
        fill = pltpu.make_async_copy(dxb, dx_out, sem.at[3])
        fill.start()
        for c in (*copies, fill):
            c.wait()

    @pl.when(st == 0)
    def _():
        copies = move((dx, dx_out))
        for b in (zb, dwb, dsb):
            b[...] = jnp.zeros_like(b)
        fills = [pltpu.make_async_copy(b, c, sem.at[1 + k]) for k, (b, c) in enumerate(((zb, z_out), (dwb, dw_out), (dsb, ds_out)))]
        for c in fills:
            c.start()
        for c in (*copies, *fills):
            c.wait()


def solution(mesh):
    act_spec = P("stage", ("dp", "tp"), None, None, None)
    kernel_spec = P("stage", None, None, "tp", None)
    short_spec = P("stage", "tp", None)
    vec_spec = P("stage", "tp")
    grad_spec = P("stage", "dp", None, None, "tp")
    any_ = pl.BlockSpec(memory_space=pl.ANY)
    vm = pl.BlockSpec(memory_space=pltpu.VMEM)

    def device_step(act_in, w_conv, w_short, gamma, beta, gamma_s, grad_z):
        by_pixel = (0, 2, 3, 1, 4)
        grads = jnp.transpose(grad_z, by_pixel).reshape(-1, B)
        call = pl.pallas_call(
            block_kernel,
            out_shape=(
                pltpu.VMEM(grads.shape, BF),
                pltpu.VMEM(act_in.shape[2:], BF),
                pltpu.VMEM(w_conv.shape[1:], F32),
                pltpu.VMEM(w_short.shape[1:], F32),
            ),
            in_specs=[any_, any_, any_, vm, vm, vm, any_],
            out_specs=(vm,) * 4,
            scratch_shapes=scratch_shapes(),
            compiler_params=pltpu.CompilerParams(vmem_limit_bytes=BIG_VMEM, has_side_effects=True, collective_id=0),
        )
        found = call(act_in[0, 0], w_conv[0], w_short[0], gamma, beta, gamma_s, grads)
        z, dx, dw, ds = pl.pallas_call(
            place_kernel,
            out_shape=tuple(jax.ShapeDtypeStruct(a.shape, a.dtype) for a in found),
            in_specs=[vm] * 4,
            out_specs=(any_,) * 4,
            scratch_shapes=[*(pltpu.VMEM(a.shape, a.dtype) for a in found), pltpu.SemaphoreType.DMA((4,))],
            compiler_params=pltpu.CompilerParams(vmem_limit_bytes=SMALL_VMEM),
        )(*found)
        z = jnp.transpose(z.reshape(1, HW, HW, IMGS, B), (0, 3, 1, 2, 4))
        return z, dx[None, None], dw[None], ds[None]

    return jax.shard_map(device_step, mesh=mesh, in_specs=(act_spec, kernel_spec, short_spec, vec_spec, vec_spec, vec_spec, grad_spec), out_specs=(grad_spec, act_spec, kernel_spec, short_spec), check_vma=False)
```
